256 devices in a mesh: ctg: 32 (over x, y, core), br: 8 (over z).
Axes of the slice: x: 4, y: 4, z: 8, core: 2. Of those that a mesh axis runs over, the one named last changes fastest.
Arguments:
- base_vm: float32 [10240], P(('ctg', 'br')), may hold values from 0.95 to 1.05
- base_va: float32 [10240], P(('ctg', 'br')), may hold values from -0.6 to 0.6
- delta_state: float32 [256, 2, 10240], P('ctg', None, 'br'), may hold values from -0.18 to 0.18
- multipliers: float32 [256, 2, 10240], P('ctg', None, 'br'), may hold values from -6 to 6
- net_inj: float32 [256, 2, 10240], P('ctg', None, 'br'), may hold values from -6 to 6
- ang_grad: float32 [256, 10240], P('ctg', 'br'), may hold values from -6 to 6
- from_bus: int32 [13312], P('br'), may hold values from 0 to 10239
- to_bus: int32 [13312], P('br'), may hold values from 0 to 10239
- status: int32 [256, 13312], P('ctg', 'br'), may hold values 0 or 1
- conduct: float32 [13312], P('br'), may hold values from 1 to 5
- suscept: float32 [13312], P('br'), may hold values from -15 to -5
- charging: float32 [13312], P('br'), may hold values from 0.1 to 0.6
- rating: float32 [13312], P('br'), may hold values from 1 to 3
- slack: float32 [256, 13312], P('ctg', 'br'), may hold values from 0.05 to 2
- zdual: float32 [256, 13312], P('ctg', 'br'), may hold values from 0.05 to 2
Outputs:
- mismatch: float32 [256, 2, 10240], P('ctg', None, 'br')
- dual_res: float32 [256, 10240], P('ctg', 'br')
- limit_res: float32 [256, 13312], P('ctg', 'br')
- ctg_norms: float32 [256, 4], P('ctg')
- total_norms: float32 [4], replicated
The draws below stay inside these ranges and needn't reach their ends.
All inputs are finite; a program needn't handle non-finite values. No bound on the sum of `status` on one device may be relied on, other than what follows from the above.
Results may differ from the reference program's by a relative error of at most 0.0003.
Values sent between devices are 32-bit elements; how exact they have to be, the bound alone decides.
A program may use at most 64 MiB of HBM per device.

```python
import math
import jax
import jax.numpy as jnp
from jax import lax

NB = 10240
NL = 13312
CTG = 256


def place_ends(drawn, rng, smallest, high):
    longest = drawn.shape.index(max(drawn.shape))
    spots = []
    for shift in (0, 1):
        where = [jax.random.randint(jax.random.fold_in(rng, axis), (), 0, length) for axis, length in enumerate(drawn.shape)]
        where[longest] = (where[longest] + shift) % drawn.shape[longest]
        spots.append(tuple(where))
    return drawn.at[spots[0]].set(smallest).at[spots[1]].set(high)


def shard_levels(key, extent, shards, low, top_value):
    def one(position, shards_of):
        draws = jax.random.uniform(jax.random.fold_in(jax.random.fold_in(key, 6), position), (shards_of,), jnp.float32, low / len(shards), top_value / len(shards))
        return jnp.repeat(jnp.exp(draws), extent[position] // shards_of).reshape((-1,) + (1,) * (len(extent) - position - 1))

    loudness = one(*shards[0])
    for cut in shards[1:]:
        loudness = loudness * one(*cut)
    return loudness


def gaussian(key, extent, width, limit, split=(), dtype=jnp.bfloat16):
    array = jax.random.normal(key, extent, jnp.float32) * width
    if len(split) > 0:
        array = shard_levels(key, extent, split, -0.22, 0.18) * array
    return jnp.clip(array, min=-limit, max=limit).astype(dtype)


def setup_inputs(seed: int = 0) -> dict:
    streams_of = jax.random.split(jax.random.key(seed), 16)
    base_vm = jnp.clip(0.95 + 0.099999964 * jax.random.uniform(streams_of[0], (NB,), jnp.float32) ** shard_levels(streams_of[0], (NB,), ((0, 256),), -0.2, 0.2), 0.95, 1.05)
    base_va = gaussian(streams_of[1], (NB,), 0.1, 0.6, ((0, 256),), jnp.float32)
    delta_state = gaussian(streams_of[2], (CTG, 2, NB), 0.03, 0.18, ((0, 32), (2, 8)), jnp.float32)
    multipliers = gaussian(streams_of[3], (CTG, 2, NB), 1.0, 6.0, ((0, 32), (2, 8)), jnp.float32)
    net_inj = gaussian(streams_of[4], (CTG, 2, NB), 1.0, 6.0, ((0, 32), (2, 8)), jnp.float32)
    ang_grad = gaussian(streams_of[5], (CTG, NB), 1.0, 6.0, ((0, 32), (1, 8)), jnp.float32)
    from_bus = place_ends(jax.random.randint(streams_of[6], (NL,), 0, NB), jax.random.fold_in(streams_of[6], 1), 0, NB - 1).astype(jnp.int32)
    to_bus = place_ends(jax.random.randint(streams_of[7], (NL,), 0, NB), jax.random.fold_in(streams_of[7], 1), 0, NB - 1).astype(jnp.int32)
    status = place_ends((jax.random.randint(streams_of[8], (CTG, NL), 0, 8) < 7).astype(jnp.int32), jax.random.fold_in(streams_of[8], 1), 0, 1)
    conduct = jnp.clip(1.0 + 4.0 * jax.random.uniform(streams_of[9], (NL,), jnp.float32) ** shard_levels(streams_of[9], (NL,), ((0, 8),), -0.2, 0.2), 1.0, 5.0)
    suscept = jnp.clip(-15.0 + 10.0 * jax.random.uniform(streams_of[10], (NL,), jnp.float32) ** shard_levels(streams_of[10], (NL,), ((0, 8),), -0.2, 0.2), -15.0, -5.0)
    charging = jnp.clip(0.1 + 0.5 * jax.random.uniform(streams_of[11], (NL,), jnp.float32) ** shard_levels(streams_of[11], (NL,), ((0, 8),), -0.2, 0.2), 0.1, 0.6)
    rating = jnp.clip(1.0 + 2.0 * jax.random.uniform(streams_of[12], (NL,), jnp.float32) ** shard_levels(streams_of[12], (NL,), ((0, 8),), -0.2, 0.2), 1.0, 3.0)
    slack = jnp.clip(jnp.exp(math.log(2.0) - 3.6888794 * jax.random.uniform(streams_of[13], (CTG, NL), jnp.float32) ** shard_levels(streams_of[13], (CTG, NL), ((0, 32), (1, 8)), -0.2, 0.2)), 0.05, 2.0)
    zdual = jnp.clip(jnp.exp(math.log(2.0) - 3.6888794 * jax.random.uniform(streams_of[14], (CTG, NL), jnp.float32) ** shard_levels(streams_of[14], (CTG, NL), ((0, 32), (1, 8)), -0.2, 0.2)), 0.05, 2.0)
    return dict(base_vm=base_vm, base_va=base_va, delta_state=delta_state, multipliers=multipliers, net_inj=net_inj, ang_grad=ang_grad, from_bus=from_bus, to_bus=to_bus, status=status, conduct=conduct, suscept=suscept, charging=charging, rating=rating, slack=slack, zdual=zdual)


def branch_flows(volt_mag, volt_ang, mult_p, mult_q, from_idx, to_idx, conduct, suscept, charging, in_service):
    volt_from = volt_mag[:, from_idx]
    volt_to = volt_mag[:, to_idx]
    angle_diff = volt_ang[:, from_idx] - volt_ang[:, to_idx]
    cos_diff = jnp.cos(angle_diff)
    sin_diff = jnp.sin(angle_diff)
    volt_prod = volt_from * volt_to
    p_from = conduct * volt_from * volt_from - volt_prod * (conduct * cos_diff + suscept * sin_diff)
    q_from = -(suscept + charging) * volt_from * volt_from - volt_prod * (conduct * sin_diff - suscept * cos_diff)
    p_to = conduct * volt_to * volt_to - volt_prod * (conduct * cos_diff - suscept * sin_diff)
    q_to = -(suscept + charging) * volt_to * volt_to + volt_prod * (conduct * sin_diff + suscept * cos_diff)
    flow_dual = volt_prod * (mult_p[:, from_idx] * (conduct * sin_diff - suscept * cos_diff) - mult_q[:, from_idx] * (conduct * cos_diff + suscept * sin_diff) + mult_p[:, to_idx] * (conduct * sin_diff + suscept * cos_diff) + mult_q[:, to_idx] * (conduct * cos_diff - suscept * sin_diff))
    at_from = jnp.stack([p_from, q_from, flow_dual], 1) * in_service[:, None, :]
    at_to = jnp.stack([p_to, q_to, -flow_dual], 1) * in_service[:, None, :]
    return (at_from, at_to)

def reference(base_vm, base_va, delta_state, multipliers, net_inj, ang_grad, from_bus, to_bus, status, conduct, suscept, charging, rating, slack, zdual):
    volt_mag = base_vm[None, :] + delta_state[:, 0]
    volt_ang = base_va[None, :] + delta_state[:, 1]
    in_service = status.astype(jnp.float32)
    at_from, at_to = branch_flows(volt_mag, volt_ang, multipliers[:, 0], multipliers[:, 1], from_bus, to_bus, conduct, suscept, charging, in_service)
    scenarios = delta_state.shape[0]
    buses = delta_state.shape[2]
    summed = jnp.zeros((scenarios, 3, buses), jnp.float32)
    summed = summed.at[:, :, from_bus].add(at_from).at[:, :, to_bus].add(at_to)
    mismatch = summed[:, :2] - net_inj
    dual_res = summed[:, 2] + ang_grad
    limit_res = in_service * (at_from[:, 0] * at_from[:, 0] + at_from[:, 1] * at_from[:, 1] + slack - rating * rating)
    complement = in_service * (zdual * slack - 0.01)
    squares = jnp.stack([lax.optimization_barrier(jnp.sum(mismatch * mismatch, axis=(1, 2))), lax.optimization_barrier(jnp.sum(dual_res * dual_res, axis=1)), lax.optimization_barrier(jnp.sum(limit_res * limit_res, axis=1)), lax.optimization_barrier(jnp.sum(complement * complement, axis=1))], 1)
    ctg_norms = jnp.sqrt(squares)
    total_norms = jnp.sqrt(lax.optimization_barrier(jnp.sum(squares, axis=0)) / scenarios)
    return (mismatch, dual_res, limit_res, ctg_norms, total_norms)
```

```python
import functools

import jax
import jax.numpy as jnp
from jax import lax
from jax.experimental import pallas as pl
from jax.experimental.pallas import tpu as pltpu
from jax.sharding import PartitionSpec as P

F32, I32, BF16 = jnp.float32, jnp.int32, jnp.bfloat16
LANES = 128
MESH = pl.DeviceIdType.MESH


def kernel(
    planes,
    ranks,
    consts,
    delta,
    mult,
    net,
    ang,
    status,
    slack,
    zdual,
    mismatch,
    dual,
    limit,
    norms,
    total,
    consts_v,
    delta_v,
    mult_v,
    net_v,
    ang_v,
    status_v,
    slack_v,
    zdual_v,
    base_z,
    base_all,
    idx_f,
    coef,
    mult_all,
    delta_all,
    net_all,
    ang_all,
    status_all,
    slack_all,
    zdual_all,
    idx,
    tables,
    ends,
    terms,
    sums,
    mis_out,
    dual_out,
    limit_out,
    sq_mine,
    sq_all,
    tot_mine,
    tot_all,
    load_sem,
    send_sem,
    recv_sem,
    base_send,
    base_recv,
    tot_send,
    tot_recv,
):
    me = lax.axis_index("ctg")
    rank = lax.axis_index("br")
    nbus = delta.shape[2]
    nline = status.shape[1]
    bus_tiles, line_tiles = nbus // LANES, nline // LANES

    loads = [
        pltpu.make_async_copy(a, b, load_sem.at[n])
        for n, (a, b) in enumerate(
            (
                (consts, consts_v),
                (mult, mult_v),
                (delta, delta_v),
                (status, status_v),
                (slack, slack_v),
                (zdual, zdual_v),
                (net, net_v),
                (ang, ang_v),
            )
        )
    ]
    for c in loads:
        c.start()

    barrier = pltpu.get_barrier_semaphore()
    for d in range(1, ranks):
        pl.semaphore_signal(barrier, 1, device_id=(me, lax.rem(rank + d, ranks)), device_id_type=MESH)

    def greet(d, carry):
        pl.semaphore_signal(barrier, 1, device_id=(lax.rem(me + d, planes), rank), device_id_type=MESH)
        return carry

    lax.fori_loop(1, planes, greet, 0)
    for c in loads:
        c.wait()
    pl.semaphore_wait(barrier, ranks - 1 + planes - 1)

    groups = (
        (lambda s: consts_v.at[6:8, 0:LANES], lambda r: base_z.at[r], base_z),
        (lambda s: consts_v.at[0:2, :], lambda r: idx_f.at[:, r, :], idx_f),
        (lambda s: mult_v.at[s], lambda r: mult_all.at[:, r, :], mult_all),
        (lambda s: delta_v.at[s], lambda r: delta_all.at[:, r, :], delta_all),
        (lambda s: consts_v.at[2:6, :], lambda r: coef.at[:, r, :], coef),
        (lambda s: status_v.at[s], lambda r: status_all.at[r], status_all),
        (lambda s: slack_v.at[s], lambda r: slack_all.at[r], slack_all),
        (lambda s: zdual_v.at[s], lambda r: zdual_all.at[r], zdual_all),
        (lambda s: net_v.at[s], lambda r: net_all.at[:, r, :], net_all),
        (lambda s: ang_v.at[s], lambda r: ang_all.at[r], ang_all),
    )

    def send(n, source, place):
        pltpu.make_async_copy(source(rank), place(rank), recv_sem.at[n]).start()
        for d in range(1, ranks):
            peer = lax.rem(rank + d, ranks)
            pltpu.make_async_remote_copy(
                src_ref=source(peer),
                dst_ref=place(rank),
                send_sem=send_sem.at[n],
                recv_sem=recv_sem.at[n],
                device_id=(me, peer),
                device_id_type=MESH,
            ).start()

    def take(n, whole):
        pltpu.make_async_copy(whole, whole, recv_sem.at[n]).wait()

    for n, (source, place, _) in enumerate(groups):
        send(n, source, place)

    take(0, base_z)
    pltpu.make_async_copy(base_z, base_all.at[me], base_recv).start()

    def spread(d, carry):
        pltpu.make_async_remote_copy(
            src_ref=base_z,
            dst_ref=base_all.at[me],
            send_sem=base_send,
            recv_sem=base_recv,
            device_id=(lax.rem(me + d, planes), rank),
            device_id_type=MESH,
        ).start()
        return carry

    lax.fori_loop(1, planes, spread, 0)

    take(1, idx_f)
    idx[...] = idx_f[...].astype(I32)
    take(2, mult_all)
    tables[2:4] = mult_all[...]
    take(3, delta_all)
    pltpu.make_async_copy(base_all, base_all, base_recv).wait()
    piece = ranks * nbus // (planes * ranks)
    per_rank = nbus // piece
    group = planes // ranks
    for q in range(2):
        tiles = [jnp.zeros((ranks, LANES), F32) for _ in range(bus_tiles)]
        lane = lax.broadcasted_iota(I32, (ranks, LANES), 1)
        for p in range(per_rank):
            rows = jnp.concatenate(
                [base_all[r * group + p // ranks, p % ranks, q : q + 1, :] for r in range(ranks)], 0
            )
            first = p * piece
            t, off = first // LANES, first % LANES
            moved = pltpu.roll(rows, off, 1) if off else rows
            tiles[t] = jnp.where((lane >= off) & (lane < off + piece), moved, tiles[t])
            if off + piece > LANES:
                tiles[t + 1] = jnp.where(lane < off + piece - LANES, moved, tiles[t + 1])
        for t in range(bus_tiles):
            cols = slice(t * LANES, (t + 1) * LANES)
            tables[q, :, cols] = tiles[t] + delta_all[q, :, cols]

    def gather(k, carry):
        cols = pl.ds(pl.multiple_of(k * LANES, LANES), LANES)
        for e in range(2):
            where_to = idx[e, :, cols]
            high, low = where_to >> 7, where_to & 127
            found = [jnp.zeros((ranks, LANES), F32) for _ in range(4)]
            for h in range(ranks * bus_tiles):
                here = high == h
                r, t = h // bus_tiles, h % bus_tiles
                for q in range(4):
                    row = jnp.broadcast_to(
                        tables[q, r : r + 1, t * LANES : (t + 1) * LANES], (ranks, LANES)
                    )
                    got = jnp.take_along_axis(row, low, axis=1, mode="promise_in_bounds")
                    found[q] = jnp.where(here, got, found[q])
            for q in range(4):
                ends[4 * e + q, :, cols] = found[q]
        return carry

    lax.fori_loop(0, line_tiles, gather, 0)

    take(4, coef)
    take(5, status_all)
    take(6, slack_all)
    take(7, zdual_all)

    def flows(k, carry):
        limit_sq, comp_sq = carry
        cols = pl.ds(pl.multiple_of(k * LANES, LANES), LANES)
        vf, af, mpf, mqf = (ends[q, :, cols] for q in range(4))
        vt, at, mpt, mqt = (ends[4 + q, :, cols] for q in range(4))
        g, b, h, rating = (coef[q, :, cols] for q in range(4))
        live = status_all[:, cols].astype(F32)
        diff = af - at
        cs, sn = jnp.cos(diff), jnp.sin(diff)
        u = vf * vt
        gcs, gsn, bcs, bsn = g * cs, g * sn, b * cs, b * sn
        pf = (g * vf * vf - u * (gcs + bsn)) * live
        qf = (-(b + h) * vf * vf - u * (gsn - bcs)) * live
        pt = (g * vt * vt - u * (gcs - bsn)) * live
        qt = (-(b + h) * vt * vt + u * (gsn + bcs)) * live
        fd = u * (mpf * (gsn - bcs) - mqf * (gcs + bsn) + mpt * (gsn + bcs) + mqt * (gcs - bsn)) * live
        terms[0, :, cols] = pf
        terms[1, :, cols] = qf
        terms[2, :, cols] = fd
        terms[3, :, cols] = pt
        terms[4, :, cols] = qt
        terms[5, :, cols] = -fd
        sl = slack_all[:, cols]
        lim = live * (pf * pf + qf * qf + sl - rating * rating)
        limit_out[:, cols] = lim
        comp = live * (zdual_all[:, cols] * sl - 0.01)
        return limit_sq + lim * lim, comp_sq + comp * comp

    zero_tile = jnp.zeros((ranks, LANES), F32)
    limit_sq, comp_sq = lax.fori_loop(0, line_tiles, flows, (zero_tile, zero_tile))

    n_limit, n_mis, n_dual, n_sq = len(groups), len(groups) + 1, len(groups) + 2, len(groups) + 3
    send(n_limit, lambda s: limit_out.at[s], lambda r: limit.at[r])

    row16 = lax.broadcasted_iota(I32, (16, LANES), 0)
    per = nbus // 256
    high_of = [((row16 & 7) * per + j).astype(F32).astype(BF16) for j in range(per)]
    low_of = row16.astype(F32).astype(BF16)
    none16, one16 = jnp.zeros((16, LANES), BF16), jnp.ones((16, LANES), BF16)
    sums[...] = jnp.zeros_like(sums)

    def scatter(k, carry):
        cols = pl.ds(pl.multiple_of(k * LANES, LANES), LANES)
        for s in range(ranks):
            left, right = [], []
            for e in range(2):
                at_bus = idx[e, s : s + 1, cols]
                high = jnp.broadcast_to((at_bus >> 8).astype(F32), (16, LANES)).astype(BF16)
                low = jnp.broadcast_to((at_bus & 255).astype(F32), (16, LANES)).astype(BF16)
                vals = []
                for r in range(3):
                    v = terms[3 * e + r, s : s + 1, cols]
                    coarse = v.astype(BF16).astype(F32)
                    fine = v - coarse
                    vals.append(
                        jnp.concatenate(
                            [jnp.broadcast_to(coarse, (8, LANES)), jnp.broadcast_to(fine, (8, LANES))], 0
                        ).astype(BF16)
                    )
                rows = []
                for j in range(per):
                    here = high == high_of[j]
                    rows += [jnp.where(here, v, none16) for v in vals]
                left.append(jnp.concatenate(rows, 0))
                right.append(
                    jnp.concatenate(
                        [jnp.where(low == low_of + BF16(16 * t), one16, none16) for t in range(16)], 0
                    )
                )
            sums[...] += lax.dot_general(
                jnp.concatenate(left, 1),
                jnp.concatenate(right, 1),
                (((1,), (1,)), ((), ())),
                preferred_element_type=F32,
            )
        return carry

    lax.fori_loop(0, line_tiles, scatter, 0)

    take(8, net_all)
    take(9, ang_all)
    mis_sq, dual_sq = jnp.zeros((ranks, 256), F32), jnp.zeros((ranks, 256), F32)
    for j in range(per):
        cols = slice(256 * j, 256 * (j + 1))
        for r in range(3):
            first = (3 * j + r) * 16
            got = sums[first : first + 8, :] + sums[first + 8 : first + 16, :]
            if r < 2:
                out = got - net_all[r, :, cols]
                mis_out[r, :, cols] = out
                mis_sq += out * out
            else:
                out = got + ang_all[:, cols]
                dual_out[:, cols] = out
                dual_sq += out * out

    parts = [mis_sq, dual_sq, limit_sq, comp_sq]
    lane8 = lax.broadcasted_iota(I32, (1, LANES), 1)
    mine = jnp.zeros((1, LANES), F32)
    for n, part in enumerate(parts):
        mine = jnp.where(lane8 == n, jnp.sum(part, keepdims=True), mine)
    sq_mine[...] = mine
    send(n_sq, lambda s: sq_mine, lambda r: sq_all.at[r])
    send(n_mis, lambda s: mis_out.at[:, s, :], lambda r: mismatch.at[r])
    send(n_dual, lambda s: dual_out.at[s], lambda r: dual.at[r])

    take(n_sq, sq_all)
    squares = sq_all[:, 0, :]
    norms[...] = jnp.sqrt(squares)[:, 0:4]
    tot_mine[...] = jnp.sum(squares, axis=0, keepdims=True)
    pltpu.make_async_copy(tot_mine, tot_all.at[me], tot_recv).start()

    def share(d, carry):
        pltpu.make_async_remote_copy(
            src_ref=tot_mine,
            dst_ref=tot_all.at[me],
            send_sem=tot_send,
            recv_sem=tot_recv,
            device_id=(lax.rem(me + d, planes), rank),
            device_id_type=MESH,
        ).start()
        return carry

    lax.fori_loop(1, planes, share, 0)
    pltpu.make_async_copy(tot_all, tot_all, tot_recv).wait()
    whole = jnp.sum(tot_all[:, 0, :], axis=0, keepdims=True)
    total[...] = jnp.sqrt(whole / (planes * ranks))

    take(n_limit, limit)
    take(n_mis, mismatch)
    take(n_dual, dual)
    for n, (_, _, dest) in enumerate(groups):
        sent(send_sem.at[n], dest, ranks)
    for n, dest in ((n_limit, limit), (n_mis, mismatch), (n_dual, dual), (n_sq, sq_all)):
        sent(send_sem.at[n], dest, ranks)
    part = base_all.at[0 : planes - 1]
    pltpu.make_async_copy(part, part, base_send).wait()
    part = tot_all.at[0 : planes - 1]
    pltpu.make_async_copy(part, part, tot_send).wait()


def sent(sem, dest, ranks):
    dim = dest.shape.index(ranks)
    part = dest.at[(slice(None),) * dim + (slice(0, ranks - 1),)]
    pltpu.make_async_copy(part, part, sem).wait()


def per_device(
    base_vm,
    base_va,
    delta_state,
    multipliers,
    net_inj,
    ang_grad,
    from_bus,
    to_bus,
    status,
    conduct,
    suscept,
    charging,
    rating,
    slack,
    zdual,
):
    planes, ranks = lax.axis_size("ctg"), lax.axis_size("br")
    nscen, _, nbus = delta_state.shape
    nline = status.shape[1]
    widen = lambda a: jnp.pad(a, (0, nline - a.shape[0]))
    consts = jnp.stack(
        [
            from_bus.astype(F32),
            to_bus.astype(F32),
            conduct,
            suscept,
            charging,
            rating,
            widen(base_vm),
            widen(base_va),
        ]
    )
    hbm = pl.BlockSpec(memory_space=pl.ANY)
    vmem = pl.BlockSpec(memory_space=pltpu.VMEM)
    V = pltpu.VMEM
    bus, line = (ranks, nbus), (ranks, nline)
    sem = pltpu.SemaphoreType.DMA
    n_groups = 14
    mismatch, dual_res, limit_res, norms, total = pl.pallas_call(
        functools.partial(kernel, planes, ranks),
        out_shape=(
            jax.ShapeDtypeStruct((nscen, 2, nbus), F32),
            jax.ShapeDtypeStruct((nscen, nbus), F32),
            jax.ShapeDtypeStruct((nscen, nline), F32),
            jax.ShapeDtypeStruct((nscen, 4), F32),
            jax.ShapeDtypeStruct((1, LANES), F32),
        ),
        in_specs=[hbm] * 8,
        out_specs=(hbm, hbm, hbm, vmem, vmem),
        scratch_shapes=[
            V((8, nline), F32),
            V((nscen, 2, nbus), F32),
            V((nscen, 2, nbus), F32),
            V((nscen, 2, nbus), F32),
            V((nscen, nbus), F32),
            V((nscen, nline), I32),
            V((nscen, nline), F32),
            V((nscen, nline), F32),
            V((ranks, 2, LANES), F32),
            V((planes, ranks, 2, LANES), F32),
            V((2,) + line, F32),
            V((4,) + line, F32),
            V((2,) + bus, F32),
            V((2,) + bus, F32),
            V((2,) + bus, F32),
            V(bus, F32),
            V(line, I32),
            V(line, F32),
            V(line, F32),
            V((2,) + line, I32),
            V((4,) + bus, F32),
            V((8,) + line, F32),
            V((6,) + line, F32),
            V((240, 256), F32),
            V((2,) + bus, F32),
            V(bus, F32),
            V(line, F32),
            V((1, LANES), F32),
            V((ranks, 1, LANES), F32),
            V((1, LANES), F32),
            V((planes, 1, LANES), F32),
            sem((8,)),
            sem((n_groups,)),
            sem((n_groups,)),
            sem,
            sem,
            sem,
            sem,
        ],
        compiler_params=pltpu.CompilerParams(collective_id=0, has_side_effects=True),
        name="residuals",
    )(consts, delta_state, multipliers, net_inj, ang_grad, status, slack, zdual)
    return mismatch, dual_res, limit_res, norms, total[0, :4]


def solution(mesh):
    placed = (
        P(("ctg", "br")),
        P(("ctg", "br")),
        P("ctg", None, "br"),
        P("ctg", None, "br"),
        P("ctg", None, "br"),
        P("ctg", "br"),
        P("br"),
        P("br"),
        P("ctg", "br"),
        P("br"),
        P("br"),
        P("br"),
        P("br"),
        P("ctg", "br"),
        P("ctg", "br"),
    )
    return jax.shard_map(
        per_device,
        mesh=mesh,
        in_specs=placed,
        out_specs=(P("ctg", None, "br"), P("ctg", "br"), P("ctg", "br"), P("ctg", None), P()),
        check_vma=False,
    )
```

```python
import functools

import jax
import jax.numpy as jnp
from jax import lax
from jax.experimental import pallas as pl
from jax.experimental.pallas import tpu as pltpu
from jax.sharding import PartitionSpec as P

F32, I32, BF16 = jnp.float32, jnp.int32, jnp.bfloat16
LANES = 128
MESH = pl.DeviceIdType.MESH


def kernel(
    planes,
    ranks,
    base_vm,
    base_va,
    from_bus,
    to_bus,
    conduct,
    suscept,
    charging,
    rating,
    delta,
    mult,
    net,
    ang,
    status,
    slack,
    zdual,
    mismatch,
    dual,
    limit,
    norms,
    total,
    lines_i,
    lines_f,
    delta_v,
    mult_v,
    net_v,
    ang_v,
    status_v,
    slack_v,
    zdual_v,
    base_v,
    base_z,
    base_all,
    idx,
    coef,
    mult_all,
    delta_all,
    net_all,
    ang_all,
    status_all,
    slack_all,
    tables,
    ends,
    terms,
    sums,
    mis_out,
    dual_out,
    limit_out,
    sq_mine,
    sq_all,
    tot_mine,
    tot_all,
    load_sem,
    send_sem,
    recv_sem,
    pass_send,
    pass_recv,
    base_send,
    base_recv,
    tot_send,
    tot_recv,
):
    me = lax.axis_index("ctg")
    rank = lax.axis_index("br")
    core = lax.rem(me, 2)
    partner = me + 1 - 2 * core
    nbus = delta.shape[2]
    nline = status.shape[1]
    bus_tiles, line_tiles = nbus // LANES, nline // LANES

    pairs = (
        (from_bus, lines_i.at[0]),
        (to_bus, lines_i.at[1]),
        (mult, mult_v),
        (delta, delta_v),
        (conduct, lines_f.at[0]),
        (suscept, lines_f.at[1]),
        (charging, lines_f.at[2]),
        (rating, lines_f.at[3]),
        (status, status_v),
        (slack, slack_v),
        (net, net_v),
        (ang, ang_v),
        (zdual, zdual_v),
    )
    loads = [pltpu.make_async_copy(a, b, load_sem.at[n]) for n, (a, b) in enumerate(pairs)]
    for c in loads:
        c.start()

    barrier = pltpu.get_barrier_semaphore()
    for d in range(1, ranks):
        pl.semaphore_signal(barrier, 1, device_id=(me, lax.rem(rank + d, ranks)), device_id_type=MESH)

    def greet(d, carry):
        pl.semaphore_signal(barrier, 1, device_id=(lax.rem(me + d, planes), rank), device_id_type=MESH)
        return carry

    lax.fori_loop(1, planes, greet, 0)
    piece = base_vm.shape[1]
    base_v[0:1, 0:piece] = base_vm[...]
    base_v[1:2, 0:piece] = base_va[...]
    for c in loads:
        c.wait()

    lane8 = lax.broadcasted_iota(I32, (ranks, LANES), 1)
    row8 = lax.broadcasted_iota(I32, (ranks, LANES), 0)
    comp_sq = jnp.zeros((ranks, LANES), F32)
    for t in range(line_tiles):
        cols = slice(t * LANES, (t + 1) * LANES)
        comp = status_v[:, cols].astype(F32) * (zdual_v[:, cols] * slack_v[:, cols] - 0.01)
        comp_sq += comp * comp
    comp_sum = jnp.sum(comp_sq, axis=1, keepdims=True)
    comp_row = jnp.sum(jnp.where(lane8 == row8 + 8, comp_sum, 0.0), axis=0, keepdims=True)

    pl.semaphore_wait(barrier, ranks - 1 + planes - 1)

    half = lambda ref: ref.at[pl.ds(2 * core, 2)]
    groups = (
        (lambda s: base_v, lambda r: base_z.at[r], base_z),
        (lambda s: lines_i.at[core], lambda r: idx.at[core, :, r, :], idx.at[core]),
        (lambda s: mult_v.at[s], lambda r: mult_all.at[:, r, :], mult_all),
        (lambda s: delta_v.at[s], lambda r: delta_all.at[:, r, :], delta_all),
        (lambda s: half(lines_f), lambda r: coef.at[pl.ds(2 * core, 2), :, r, :], half(coef)),
        (lambda s: status_v.at[s], lambda r: status_all.at[r], status_all),
        (lambda s: slack_v.at[s], lambda r: slack_all.at[r], slack_all),
        (lambda s: net_v.at[s], lambda r: net_all.at[:, r, :], net_all),
        (lambda s: ang_v.at[s], lambda r: ang_all.at[r], ang_all),
    )

    def send(n, source, place):
        pltpu.make_async_copy(source(rank), place(rank), recv_sem.at[n]).start()
        for d in range(1, ranks):
            peer = lax.rem(rank + d, ranks)
            pltpu.make_async_remote_copy(
                src_ref=source(peer),
                dst_ref=place(rank),
                send_sem=send_sem.at[n],
                recv_sem=recv_sem.at[n],
                device_id=(me, peer),
                device_id_type=MESH,
            ).start()

    def take(n, whole):
        pltpu.make_async_copy(whole, whole, recv_sem.at[n]).wait()

    for n, (source, place, _) in enumerate(groups):
        send(n, source, place)

    def across(n, mine, theirs):
        out = pltpu.make_async_remote_copy(
            src_ref=mine,
            dst_ref=mine,
            send_sem=pass_send.at[n],
            recv_sem=pass_recv.at[n],
            device_id=(partner, rank),
            device_id_type=MESH,
        )
        out.start()
        return out, pltpu.make_async_copy(theirs, theirs, pass_recv.at[n])

    take(0, base_z)
    group = planes // ranks
    home = base_all.at[lax.rem(me, group), :, :, me // group, :]
    pltpu.make_async_copy(base_z, home, base_recv).start()

    def spread(d, carry):
        pltpu.make_async_remote_copy(
            src_ref=base_z,
            dst_ref=home,
            send_sem=base_send,
            recv_sem=base_recv,
            device_id=(lax.rem(me + d, planes), rank),
            device_id_type=MESH,
        ).start()
        return carry

    lax.fori_loop(1, planes, spread, 0)

    take(1, idx.at[core])
    idx_out, idx_in = across(0, idx.at[core], idx.at[1 - core])
    take(2, mult_all)
    idx_in.wait()

    def look_up(first, k):
        for e in range(2):
            where_to = idx[e, k]
            high, low = where_to >> 7, where_to & 127
            found = [jnp.zeros((ranks, LANES), F32) for _ in range(2)]
            for h in range(ranks * bus_tiles):
                here = high == h
                r, t = h // bus_tiles, h % bus_tiles
                for q in range(2):
                    src = mult_all if first else tables
                    row = jnp.broadcast_to(src[q, r : r + 1, t * LANES : (t + 1) * LANES], (ranks, LANES))
                    got = jnp.take_along_axis(row, low, axis=1, mode="promise_in_bounds")
                    found[q] = jnp.where(here, got, found[q])
            for q in range(2):
                ends[4 * e + 2 * first + q, k] = found[q]

    def gather_mult(k, carry):
        look_up(1, k)
        return carry

    lax.fori_loop(0, line_tiles, gather_mult, 0)

    take(3, delta_all)
    pltpu.make_async_copy(base_all, base_all, base_recv).wait()
    for q in range(2):
        tiles = [jnp.zeros((ranks, LANES), F32) for _ in range(bus_tiles)]
        for p in range(nbus // piece):
            rows = base_all[p // ranks, p % ranks, q]
            t, off = p * piece // LANES, p * piece % LANES
            moved = pltpu.roll(rows, off, 1) if off else rows
            tiles[t] = jnp.where((lane8 >= off) & (lane8 < off + piece), moved, tiles[t])
            if off + piece > LANES:
                tiles[t + 1] = jnp.where(lane8 < off + piece - LANES, moved, tiles[t + 1])
        for t in range(bus_tiles):
            cols = slice(t * LANES, (t + 1) * LANES)
            tables[q, :, cols] = tiles[t] + delta_all[q, :, cols]

    take(4, half(coef))
    coef_out, coef_in = across(1, half(coef), coef.at[pl.ds(2 - 2 * core, 2)])

    def gather_volt(k, carry):
        look_up(0, k)
        return carry

    lax.fori_loop(0, line_tiles, gather_volt, 0)

    coef_in.wait()
    take(5, status_all)

    def flows(k, carry):
        cols = pl.ds(pl.multiple_of(k * LANES, LANES), LANES)
        vf, af, mpf, mqf = (ends[q, k] for q in range(4))
        vt, at, mpt, mqt = (ends[4 + q, k] for q in range(4))
        g, b, h = (coef[q, k] for q in range(3))
        live = status_all[:, cols].astype(F32)
        diff = af - at
        cs, sn = jnp.cos(diff), jnp.sin(diff)
        u = vf * vt
        gcs, gsn, bcs, bsn = g * cs, g * sn, b * cs, b * sn
        pf = (g * vf * vf - u * (gcs + bsn)) * live
        qf = (-(b + h) * vf * vf - u * (gsn - bcs)) * live
        pt = (g * vt * vt - u * (gcs - bsn)) * live
        qt = (-(b + h) * vt * vt + u * (gsn + bcs)) * live
        fd = u * (mpf * (gsn - bcs) - mqf * (gcs + bsn) + mpt * (gsn + bcs) + mqt * (gcs - bsn)) * live
        for n, v in enumerate((pf, qf, fd, pt, qt, -fd)):
            terms[n, k] = v
        return carry

    lax.fori_loop(0, line_tiles, flows, 0)

    take(6, slack_all)
    limit_sq = jnp.zeros((ranks, LANES), F32)
    for k in range(line_tiles):
        cols = slice(k * LANES, (k + 1) * LANES)
        pf, qf = terms[0, k], terms[1, k]
        live = status_all[:, cols].astype(F32)
        lim = live * (pf * pf + qf * qf + slack_all[:, cols] - coef[3, k] * coef[3, k])
        limit_out[:, cols] = lim
        limit_sq += lim * lim

    n_limit, n_mis, n_dual, n_sq = (len(groups) + n for n in range(4))
    send(n_limit, lambda s: limit_out.at[s], lambda r: limit.at[r])

    row16 = lax.broadcasted_iota(I32, (16, LANES), 0)
    per = nbus // 256
    high_of = [((row16 & 7) * per + j).astype(F32).astype(BF16) for j in range(per)]
    low_of = row16.astype(F32).astype(BF16)
    none16, one16 = jnp.zeros((16, LANES), BF16), jnp.ones((16, LANES), BF16)
    sums[...] = jnp.zeros_like(sums)

    def scatter(k, carry):
        for s in range(ranks):
            left, right = [], []
            for e in range(2):
                at_bus = idx[e, k, s : s + 1, :]
                high = jnp.broadcast_to((at_bus >> 8).astype(F32), (16, LANES)).astype(BF16)
                low = jnp.broadcast_to((at_bus & 255).astype(F32), (16, LANES)).astype(BF16)
                vals = []
                for r in range(3):
                    v = terms[3 * e + r, k, s : s + 1, :]
                    coarse = v.astype(BF16).astype(F32)
                    fine = v - coarse
                    vals.append(
                        jnp.concatenate(
                            [jnp.broadcast_to(coarse, (8, LANES)), jnp.broadcast_to(fine, (8, LANES))], 0
                        ).astype(BF16)
                    )
                rows = []
                for j in range(per):
                    here = high == high_of[j]
                    rows += [jnp.where(here, v, none16) for v in vals]
                left.append(jnp.concatenate(rows, 0))
                right.append(
                    jnp.concatenate(
                        [jnp.where(low == low_of + BF16(16 * t), one16, none16) for t in range(16)], 0
                    )
                )
            sums[...] += lax.dot_general(
                jnp.concatenate(left, 1),
                jnp.concatenate(right, 1),
                (((1,), (1,)), ((), ())),
                preferred_element_type=F32,
            )
        return carry

    lax.fori_loop(0, line_tiles, scatter, 0)

    take(7, net_all)
    take(8, ang_all)
    mis_sq, dual_sq = jnp.zeros((ranks, 256), F32), jnp.zeros((ranks, 256), F32)
    for j in range(per):
        cols = slice(256 * j, 256 * (j + 1))
        for r in range(3):
            first = (3 * j + r) * 16
            got = sums[first : first + 8, :] + sums[first + 8 : first + 16, :]
            if r < 2:
                out = got - net_all[r, :, cols]
                mis_out[r, :, cols] = out
                mis_sq += out * out
            else:
                out = got + ang_all[:, cols]
                dual_out[:, cols] = out
                dual_sq += out * out

    mine = comp_row
    for n, part in enumerate((mis_sq, dual_sq, limit_sq)):
        mine = jnp.where(lane8[0:1] == n, jnp.sum(part, keepdims=True), mine)
    sq_mine[...] = mine
    send(n_sq, lambda s: sq_mine, lambda r: sq_all.at[r])
    send(n_mis, lambda s: mis_out.at[:, s, :], lambda r: mismatch.at[r])
    send(n_dual, lambda s: dual_out.at[s], lambda r: dual.at[r])

    take(n_sq, sq_all)
    every = sq_all[:, 0, :]
    comp_all = jnp.sum(every, axis=0, keepdims=True)
    comp_of = jnp.sum(jnp.where(lane8 == row8 + 8, comp_all, 0.0), axis=1, keepdims=True)
    squares = jnp.where(lane8 == 3, comp_of, jnp.where(lane8 < 3, every, 0.0))
    tot_mine[...] = jnp.sum(squares, axis=0, keepdims=True)
    pltpu.make_async_copy(tot_mine, tot_all.at[me], tot_recv).start()

    def share(d, carry):
        pltpu.make_async_remote_copy(
            src_ref=tot_mine,
            dst_ref=tot_all.at[me],
            send_sem=tot_send,
            recv_sem=tot_recv,
            device_id=(lax.rem(me + d, planes), rank),
            device_id_type=MESH,
        ).start()
        return carry

    lax.fori_loop(1, planes, share, 0)
    norms[...] = jnp.sqrt(squares)
    take(n_limit, limit)
    take(n_mis, mismatch)
    take(n_dual, dual)
    idx_out.wait_send()
    coef_out.wait_send()
    for n, (_, _, dest) in enumerate(groups):
        sent(send_sem.at[n], dest, ranks)
    for n, dest in ((n_limit, limit), (n_mis, mismatch), (n_dual, dual), (n_sq, sq_all)):
        sent(send_sem.at[n], dest, ranks)
    part = base_all.at[:, :, :, 0 : ranks - 1, :]
    pltpu.make_async_copy(part, part, base_send).wait()
    part = base_all.at[0 : group - 1, :, :, ranks - 1, :]
    pltpu.make_async_copy(part, part, base_send).wait()
    pltpu.make_async_copy(tot_all, tot_all, tot_recv).wait()
    whole = jnp.sum(tot_all[:, 0, :], axis=0, keepdims=True)
    total[...] = jnp.sqrt(whole / (planes * ranks))
    part = tot_all.at[0 : planes - 1]
    pltpu.make_async_copy(part, part, tot_send).wait()


def sent(sem, dest, ranks):
    dim = len(dest.shape) - 1 - dest.shape[::-1].index(ranks)
    part = dest.at[(slice(None),) * dim + (slice(0, ranks - 1),)]
    pltpu.make_async_copy(part, part, sem).wait()


def hand_out(norms, total, mis, dual, limit, norms_out, total_out, mis_out, dual_out, limit_out, sem):
    pairs = ((mis, mis_out), (dual, dual_out), (limit, limit_out))
    copies = [pltpu.make_async_copy(a, b, sem.at[n]) for n, (a, b) in enumerate(pairs)]
    for c in copies:
        c.start()
    norms_out[...] = norms[...].T[0:4, :]
    total_out[...] = total[:, 0:4]
    for c in copies:
        c.wait()


def per_device(
    base_vm,
    base_va,
    delta_state,
    multipliers,
    net_inj,
    ang_grad,
    from_bus,
    to_bus,
    status,
    conduct,
    suscept,
    charging,
    rating,
    slack,
    zdual,
):
    planes, ranks = lax.axis_size("ctg"), lax.axis_size("br")
    nscen, _, nbus = delta_state.shape
    nline = status.shape[1]
    tiles = nline // LANES
    hbm = pl.BlockSpec(memory_space=pl.ANY)
    vmem = pl.BlockSpec(memory_space=pltpu.VMEM)
    V = pltpu.VMEM
    bus, line, deep = (ranks, nbus), (ranks, nline), (tiles, ranks, LANES)
    sem = pltpu.SemaphoreType.DMA
    row = lambda a: a.reshape(1, -1)
    grid = lambda a: a.reshape(tiles, LANES)
    results = pl.pallas_call(
        functools.partial(kernel, planes, ranks),
        out_shape=(
            V((nscen, 2, nbus), F32),
            V((nscen, nbus), F32),
            V((nscen, nline), F32),
            V((nscen, LANES), F32),
            V((1, LANES), F32),
        ),
        in_specs=[vmem] * 2 + [hbm] * 13,
        out_specs=(vmem,) * 5,
        scratch_shapes=[
            V((2, tiles, LANES), I32),
            V((4, tiles, LANES), F32),
            V((nscen, 2, nbus), F32),
            V((nscen, 2, nbus), F32),
            V((nscen, 2, nbus), F32),
            V((nscen, nbus), F32),
            V((nscen, nline), I32),
            V((nscen, nline), F32),
            V((nscen, nline), F32),
            V((2, LANES), F32),
            V((ranks, 2, LANES), F32),
            V((planes // ranks, ranks, 2, ranks, LANES), F32),
            V((2,) + deep, I32),
            V((4,) + deep, F32),
            V((2,) + bus, F32),
            V((2,) + bus, F32),
            V((2,) + bus, F32),
            V(bus, F32),
            V(line, I32),
            V(line, F32),
            V((2,) + bus, F32),
            V((8,) + deep, F32),
            V((6,) + deep, F32),
            V((240, 256), F32),
            V((2,) + bus, F32),
            V(bus, F32),
            V(line, F32),
            V((1, LANES), F32),
            V((ranks, 1, LANES), F32),
            V((1, LANES), F32),
            V((planes, 1, LANES), F32),
            sem((13,)),
            sem((13,)),
            sem((13,)),
            sem((2,)),
            sem((2,)),
            sem,
            sem,
            sem,
            sem,
        ],
        compiler_params=pltpu.CompilerParams(collective_id=0, has_side_effects=True),
        name="residuals",
    )(
        row(base_vm),
        row(base_va),
        grid(from_bus),
        grid(to_bus),
        grid(conduct),
        grid(suscept),
        grid(charging),
        grid(rating),
        delta_state,
        multipliers,
        net_inj,
        ang_grad,
        status,
        slack,
        zdual,
    )
    mis, dual, limit, norms, total = (pltpu.with_memory_space_constraint(r, V) for r in results)
    norms, total, mis, dual, limit = pl.pallas_call(
        hand_out,
        out_shape=(
            jax.ShapeDtypeStruct((4, nscen), F32),
            jax.ShapeDtypeStruct((1, 4), F32),
            jax.ShapeDtypeStruct((nscen, 2, nbus), F32),
            jax.ShapeDtypeStruct((nscen, nbus), F32),
            jax.ShapeDtypeStruct((nscen, nline), F32),
        ),
        in_specs=[vmem] * 5,
        out_specs=(vmem, vmem, hbm, hbm, hbm),
        scratch_shapes=[sem((3,))],
        name="hand_out",
    )(norms, total, mis, dual, limit)
    return mis, dual, limit, norms.T, total.reshape(4)


def solution(mesh):
    placed = (
        P(("ctg", "br")),
        P(("ctg", "br")),
        P("ctg", None, "br"),
        P("ctg", None, "br"),
        P("ctg", None, "br"),
        P("ctg", "br"),
        P("br"),
        P("br"),
        P("ctg", "br"),
        P("br"),
        P("br"),
        P("br"),
        P("br"),
        P("ctg", "br"),
        P("ctg", "br"),
    )
    return jax.shard_map(
        per_device,
        mesh=mesh,
        in_specs=placed,
        out_specs=(P("ctg", None, "br"), P("ctg", "br"), P("ctg", "br"), P("ctg", None), P()),
        check_vma=False,
    )
```

```python
import functools

import jax
import jax.numpy as jnp
from jax import lax
from jax.experimental import pallas as pl
from jax.experimental.pallas import tpu as pltpu
from jax.sharding import PartitionSpec as P

F32, I32, BF16 = jnp.float32, jnp.int32, jnp.bfloat16
LANES = 128
MESH = pl.DeviceIdType.MESH


def kernel(
    planes,
    ranks,
    base_vm,
    base_va,
    from_bus,
    to_bus,
    conduct,
    suscept,
    charging,
    rating,
    delta,
    mult,
    net,
    ang,
    status,
    slack,
    zdual,
    mismatch,
    dual,
    limit,
    norms,
    total,
    lines_i,
    lines_f,
    delta_v,
    mult_v,
    net_v,
    ang_v,
    status_v,
    slack_v,
    zdual_v,
    base_v,
    base_z,
    base_all,
    idx,
    coef,
    mult_all,
    delta_all,
    net_all,
    ang_all,
    status_all,
    slack_all,
    angles,
    stacked,
    ends,
    terms,
    sums,
    mis_out,
    dual_out,
    limit_out,
    sq_mine,
    sq_all,
    tot_mine,
    tot_all,
    load_sem,
    send_sem,
    recv_sem,
    pass_send,
    pass_recv,
    base_send,
    base_recv,
    tot_send,
    tot_recv,
):
    me = lax.axis_index("ctg")
    rank = lax.axis_index("br")
    core = lax.rem(me, 2)
    partner = me + 1 - 2 * core
    nbus = delta.shape[2]
    nline = status.shape[1]
    bus_tiles, line_tiles = nbus // LANES, nline // LANES

    pairs = (
        (from_bus, lines_i.at[0]),
        (to_bus, lines_i.at[1]),
        (mult, mult_v),
        (delta, delta_v),
        (conduct, lines_f.at[0]),
        (suscept, lines_f.at[1]),
        (charging, lines_f.at[2]),
        (rating, lines_f.at[3]),
        (status, status_v),
        (slack, slack_v),
        (net, net_v),
        (ang, ang_v),
        (zdual, zdual_v),
    )
    loads = [pltpu.make_async_copy(a, b, load_sem.at[n]) for n, (a, b) in enumerate(pairs)]
    for c in loads:
        c.start()

    barrier = pltpu.get_barrier_semaphore()
    for d in range(1, ranks):
        pl.semaphore_signal(barrier, 1, device_id=(me, lax.rem(rank + d, ranks)), device_id_type=MESH)

    def greet(d, carry):
        pl.semaphore_signal(barrier, 1, device_id=(lax.rem(me + d, planes), rank), device_id_type=MESH)
        return carry

    lax.fori_loop(1, planes, greet, 0)
    piece = base_vm.shape[1]
    base_v[0:1, 0:piece] = base_vm[...]
    base_v[1:2, 0:piece] = base_va[...]
    for c in loads:
        c.wait()

    lane8 = lax.broadcasted_iota(I32, (ranks, LANES), 1)
    row8 = lax.broadcasted_iota(I32, (ranks, LANES), 0)
    comp_sq = jnp.zeros((ranks, LANES), F32)
    for t in range(line_tiles):
        cols = slice(t * LANES, (t + 1) * LANES)
        comp = status_v[:, cols].astype(F32) * (zdual_v[:, cols] * slack_v[:, cols] - 0.01)
        comp_sq += comp * comp
    comp_sum = jnp.sum(comp_sq, axis=1, keepdims=True)
    comp_row = jnp.sum(jnp.where(lane8 == row8 + 8, comp_sum, 0.0), axis=0, keepdims=True)

    pl.semaphore_wait(barrier, ranks - 1 + planes - 1)

    half = lambda ref: ref.at[pl.ds(2 * core, 2)]
    groups = (
        (lambda s: base_v, lambda r: base_z.at[r], base_z),
        (lambda s: lines_i.at[core], lambda r: idx.at[core, :, r, :], idx.at[core]),
        (lambda s: mult_v.at[s], lambda r: mult_all.at[:, r, :], mult_all),
        (lambda s: delta_v.at[s], lambda r: delta_all.at[:, r, :], delta_all),
        (lambda s: half(lines_f), lambda r: coef.at[pl.ds(2 * core, 2), :, r, :], half(coef)),
        (lambda s: status_v.at[s], lambda r: status_all.at[r], status_all),
        (lambda s: slack_v.at[s], lambda r: slack_all.at[r], slack_all),
        (lambda s: net_v.at[s], lambda r: net_all.at[:, r, :], net_all),
        (lambda s: ang_v.at[s], lambda r: ang_all.at[r], ang_all),
    )

    def send(n, source, place):
        pltpu.make_async_copy(source(rank), place(rank), recv_sem.at[n]).start()
        for d in range(1, ranks):
            peer = lax.rem(rank + d, ranks)
            pltpu.make_async_remote_copy(
                src_ref=source(peer),
                dst_ref=place(rank),
                send_sem=send_sem.at[n],
                recv_sem=recv_sem.at[n],
                device_id=(me, peer),
                device_id_type=MESH,
            ).start()

    def take(n, whole):
        pltpu.make_async_copy(whole, whole, recv_sem.at[n]).wait()

    for n, (source, place, _) in enumerate(groups):
        send(n, source, place)

    def across(n, mine, theirs):
        out = pltpu.make_async_remote_copy(
            src_ref=mine,
            dst_ref=mine,
            send_sem=pass_send.at[n],
            recv_sem=pass_recv.at[n],
            device_id=(partner, rank),
            device_id_type=MESH,
        )
        out.start()
        return out, pltpu.make_async_copy(theirs, theirs, pass_recv.at[n])

    take(0, base_z)
    group = planes // ranks
    home = base_all.at[lax.rem(me, group), :, :, me // group, :]
    pltpu.make_async_copy(base_z, home, base_recv).start()

    def spread(d, carry):
        pltpu.make_async_remote_copy(
            src_ref=base_z,
            dst_ref=home,
            send_sem=base_send,
            recv_sem=base_recv,
            device_id=(lax.rem(me + d, planes), rank),
            device_id_type=MESH,
        ).start()
        return carry

    lax.fori_loop(1, planes, spread, 0)

    take(1, idx.at[core])
    idx_out, idx_in = across(0, idx.at[core], idx.at[1 - core])
    take(2, mult_all)
    idx_in.wait()

    row16 = lax.broadcasted_iota(I32, (16, LANES), 0)
    ramp16 = row16.astype(F32).astype(BF16)
    none16, one16 = jnp.zeros((16, LANES), BF16), jnp.ones((16, LANES), BF16)
    high_row = [row8 * bus_tiles + t for t in range(bus_tiles)]
    n_rows = ranks * bus_tiles

    def one_hot(low, tiles):
        low = jnp.broadcast_to(low.astype(F32), (16, LANES)).astype(BF16)
        return jnp.concatenate(
            [jnp.where(low == ramp16 + BF16(16 * t), one16, none16) for t in range(tiles)], 0
        )

    def stack(q, tile):
        for t in range(0, bus_tiles, 2):
            both = jnp.concatenate([tile(t), tile(t + 1)], 0)
            coarse = both.astype(BF16)
            rows = slice(q * n_rows + ranks * t, q * n_rows + ranks * (t + 2))
            stacked[rows, 0:LANES] = coarse
            stacked[rows, LANES:] = (both - coarse.astype(F32)).astype(BF16)

    def by_matmul(k, count, store):
        for e in range(2):
            out = [jnp.zeros((ranks, LANES), F32) for _ in range(count)]
            for s in range(0, ranks, 2):
                hot, high = [], []
                for n in range(2):
                    bus = idx[e, k, s + n : s + n + 1, :]
                    high.append(jnp.broadcast_to(bus >> 7, (ranks, LANES)))
                    hot.append(one_hot(bus & 127, LANES // 16))
                hot = jnp.concatenate(hot, 1)
                rows = jnp.dot(
                    stacked[0 : count * n_rows, :],
                    jnp.concatenate([hot, hot], 0),
                    preferred_element_type=F32,
                )
                for n in range(2):
                    for q in range(count):
                        acc = jnp.zeros((ranks, LANES), F32)
                        for t in range(bus_tiles):
                            first = q * n_rows + ranks * t
                            part = rows[first : first + ranks, n * LANES : (n + 1) * LANES]
                            acc = jnp.where(high[n] == high_row[t], part, acc)
                        for step in (4, 2, 1):
                            acc = acc + pltpu.roll(acc, step, 0)
                        out[q] = jnp.where(row8 == s + n, acc, out[q])
            for q in range(count):
                store(e, q, out[q])

    def by_permute(k, store):
        for e in range(2):
            bus = idx[e, k]
            high, low = bus >> 7, bus & 127
            found = jnp.zeros((ranks, LANES), F32)
            for h in range(n_rows):
                r, t = h // bus_tiles, h % bus_tiles
                row = jnp.broadcast_to(angles[r : r + 1, t * LANES : (t + 1) * LANES], (ranks, LANES))
                got = jnp.take_along_axis(row, low, axis=1, mode="promise_in_bounds")
                found = jnp.where(high == h, got, found)
            store(e, found)

    for q in range(2):
        stack(q, lambda t: mult_all[q, :, t * LANES : (t + 1) * LANES])

    def gather_mult(k, carry):
        def store(e, q, value):
            ends[4 * e + 2 + q, k] = value

        by_matmul(k, 2, store)
        return carry

    lax.fori_loop(0, line_tiles, gather_mult, 0)

    take(3, delta_all)
    pltpu.make_async_copy(base_all, base_all, base_recv).wait()
    for q in range(2):
        tiles = [jnp.zeros((ranks, LANES), F32) for _ in range(bus_tiles)]
        for p in range(nbus // piece):
            rows = base_all[p // ranks, p % ranks, q]
            t, off = p * piece // LANES, p * piece % LANES
            moved = pltpu.roll(rows, off, 1) if off else rows
            tiles[t] = jnp.where((lane8 >= off) & (lane8 < off + piece), moved, tiles[t])
            if off + piece > LANES:
                tiles[t + 1] = jnp.where(lane8 < off + piece - LANES, moved, tiles[t + 1])
        for t in range(bus_tiles):
            cols = slice(t * LANES, (t + 1) * LANES)
            tiles[t] = tiles[t] + delta_all[q, :, cols]
            if q == 1:
                angles[:, cols] = tiles[t]
        if q == 0:
            stack(0, lambda t: tiles[t] - 1.0)

    take(4, half(coef))
    coef_out, coef_in = across(1, half(coef), coef.at[pl.ds(2 - 2 * core, 2)])

    def gather_volt(k, carry):
        def store_vm(e, q, value):
            ends[4 * e, k] = value + 1.0

        def store_va(e, value):
            ends[4 * e + 1, k] = value

        by_permute(k, store_va)
        by_matmul(k, 1, store_vm)
        return carry

    lax.fori_loop(0, line_tiles, gather_volt, 0)

    coef_in.wait()
    take(5, status_all)

    def flows(k, carry):
        cols = pl.ds(pl.multiple_of(k * LANES, LANES), LANES)
        vf, af, mpf, mqf = (ends[q, k] for q in range(4))
        vt, at, mpt, mqt = (ends[4 + q, k] for q in range(4))
        g, b, h = (coef[q, k] for q in range(3))
        live = status_all[:, cols].astype(F32)
        diff = af - at
        cs, sn = jnp.cos(diff), jnp.sin(diff)
        u = vf * vt
        gcs, gsn, bcs, bsn = g * cs, g * sn, b * cs, b * sn
        pf = (g * vf * vf - u * (gcs + bsn)) * live
        qf = (-(b + h) * vf * vf - u * (gsn - bcs)) * live
        pt = (g * vt * vt - u * (gcs - bsn)) * live
        qt = (-(b + h) * vt * vt + u * (gsn + bcs)) * live
        fd = u * (mpf * (gsn - bcs) - mqf * (gcs + bsn) + mpt * (gsn + bcs) + mqt * (gcs - bsn)) * live
        for n, v in enumerate((pf, qf, fd, pt, qt, -fd)):
            terms[n, k] = v
        return carry

    lax.fori_loop(0, line_tiles, flows, 0)

    take(6, slack_all)
    limit_sq = jnp.zeros((ranks, LANES), F32)
    for k in range(line_tiles):
        cols = slice(k * LANES, (k + 1) * LANES)
        pf, qf = terms[0, k], terms[1, k]
        live = status_all[:, cols].astype(F32)
        lim = live * (pf * pf + qf * qf + slack_all[:, cols] - coef[3, k] * coef[3, k])
        limit_out[:, cols] = lim
        limit_sq += lim * lim

    n_limit, n_mis, n_dual, n_sq = (len(groups) + n for n in range(4))
    send(n_limit, lambda s: limit_out.at[s], lambda r: limit.at[r])

    per = nbus // 256
    high_of = [((row16 & 7) * per + j).astype(F32).astype(BF16) for j in range(per)]
    sums[...] = jnp.zeros_like(sums)

    def scatter(k, carry):
        for s in range(ranks):
            left, right = [], []
            for e in range(2):
                at_bus = idx[e, k, s : s + 1, :]
                high = jnp.broadcast_to((at_bus >> 8).astype(F32), (16, LANES)).astype(BF16)
                vals = []
                for r in range(3):
                    v = terms[3 * e + r, k, s : s + 1, :]
                    coarse = v.astype(BF16).astype(F32)
                    fine = v - coarse
                    vals.append(
                        jnp.concatenate(
                            [jnp.broadcast_to(coarse, (8, LANES)), jnp.broadcast_to(fine, (8, LANES))], 0
                        ).astype(BF16)
                    )
                rows = []
                for j in range(per):
                    here = high == high_of[j]
                    rows += [jnp.where(here, v, none16) for v in vals]
                left.append(jnp.concatenate(rows, 0))
                right.append(one_hot(at_bus & 255, 16))
            sums[...] += lax.dot_general(
                jnp.concatenate(left, 1),
                jnp.concatenate(right, 1),
                (((1,), (1,)), ((), ())),
                preferred_element_type=F32,
            )
        return carry

    lax.fori_loop(0, line_tiles, scatter, 0)

    take(7, net_all)
    take(8, ang_all)
    mis_sq, dual_sq = jnp.zeros((ranks, 256), F32), jnp.zeros((ranks, 256), F32)
    for j in range(per):
        cols = slice(256 * j, 256 * (j + 1))
        for r in range(3):
            first = (3 * j + r) * 16
            got = sums[first : first + 8, :] + sums[first + 8 : first + 16, :]
            if r < 2:
                out = got - net_all[r, :, cols]
                mis_out[r, :, cols] = out
                mis_sq += out * out
            else:
                out = got + ang_all[:, cols]
                dual_out[:, cols] = out
                dual_sq += out * out

    mine = comp_row
    for n, part in enumerate((mis_sq, dual_sq, limit_sq)):
        mine = jnp.where(lane8[0:1] == n, jnp.sum(part, keepdims=True), mine)
    sq_mine[...] = mine
    send(n_sq, lambda s: sq_mine, lambda r: sq_all.at[r])
    send(n_mis, lambda s: mis_out.at[:, s, :], lambda r: mismatch.at[r])
    send(n_dual, lambda s: dual_out.at[s], lambda r: dual.at[r])

    take(n_sq, sq_all)
    every = sq_all[:, 0, :]
    comp_all = jnp.sum(every, axis=0, keepdims=True)
    comp_of = jnp.sum(jnp.where(lane8 == row8 + 8, comp_all, 0.0), axis=1, keepdims=True)
    squares = jnp.where(lane8 == 3, comp_of, jnp.where(lane8 < 3, every, 0.0))
    tot_mine[...] = jnp.sum(squares, axis=0, keepdims=True)
    pltpu.make_async_copy(tot_mine, tot_all.at[me], tot_recv).start()

    def share(d, carry):
        pltpu.make_async_remote_copy(
            src_ref=tot_mine,
            dst_ref=tot_all.at[me],
            send_sem=tot_send,
            recv_sem=tot_recv,
            device_id=(lax.rem(me + d, planes), rank),
            device_id_type=MESH,
        ).start()
        return carry

    lax.fori_loop(1, planes, share, 0)
    norms[...] = jnp.sqrt(squares)
    take(n_limit, limit)
    take(n_mis, mismatch)
    take(n_dual, dual)
    idx_out.wait_send()
    coef_out.wait_send()
    for n, (_, _, dest) in enumerate(groups):
        sent(send_sem.at[n], dest, ranks)
    for n, dest in ((n_limit, limit), (n_mis, mismatch), (n_dual, dual), (n_sq, sq_all)):
        sent(send_sem.at[n], dest, ranks)
    part = base_all.at[:, :, :, 0 : ranks - 1, :]
    pltpu.make_async_copy(part, part, base_send).wait()
    part = base_all.at[0 : group - 1, :, :, ranks - 1, :]
    pltpu.make_async_copy(part, part, base_send).wait()
    pltpu.make_async_copy(tot_all, tot_all, tot_recv).wait()
    whole = jnp.sum(tot_all[:, 0, :], axis=0, keepdims=True)
    total[...] = jnp.sqrt(whole / (planes * ranks))
    part = tot_all.at[0 : planes - 1]
    pltpu.make_async_copy(part, part, tot_send).wait()


def sent(sem, dest, ranks):
    dim = len(dest.shape) - 1 - dest.shape[::-1].index(ranks)
    part = dest.at[(slice(None),) * dim + (slice(0, ranks - 1),)]
    pltpu.make_async_copy(part, part, sem).wait()


def hand_out(norms, total, mis, dual, limit, norms_out, total_out, mis_out, dual_out, limit_out, sem):
    pairs = ((mis, mis_out), (dual, dual_out), (limit, limit_out))
    copies = [pltpu.make_async_copy(a, b, sem.at[n]) for n, (a, b) in enumerate(pairs)]
    for c in copies:
        c.start()
    norms_out[...] = norms[...].T[0:4, :]
    total_out[...] = total[:, 0:4]
    for c in copies:
        c.wait()


def per_device(
    base_vm,
    base_va,
    delta_state,
    multipliers,
    net_inj,
    ang_grad,
    from_bus,
    to_bus,
    status,
    conduct,
    suscept,
    charging,
    rating,
    slack,
    zdual,
):
    planes, ranks = lax.axis_size("ctg"), lax.axis_size("br")
    nscen, _, nbus = delta_state.shape
    nline = status.shape[1]
    tiles = nline // LANES
    hbm = pl.BlockSpec(memory_space=pl.ANY)
    vmem = pl.BlockSpec(memory_space=pltpu.VMEM)
    V = pltpu.VMEM
    bus, line, deep = (ranks, nbus), (ranks, nline), (tiles, ranks, LANES)
    sem = pltpu.SemaphoreType.DMA
    row = lambda a: a.reshape(1, -1)
    grid = lambda a: a.reshape(tiles, LANES)
    results = pl.pallas_call(
        functools.partial(kernel, planes, ranks),
        out_shape=(
            V((nscen, 2, nbus), F32),
            V((nscen, nbus), F32),
            V((nscen, nline), F32),
            V((nscen, LANES), F32),
            V((1, LANES), F32),
        ),
        in_specs=[vmem] * 2 + [hbm] * 13,
        out_specs=(vmem,) * 5,
        scratch_shapes=[
            V((2, tiles, LANES), I32),
            V((4, tiles, LANES), F32),
            V((nscen, 2, nbus), F32),
            V((nscen, 2, nbus), F32),
            V((nscen, 2, nbus), F32),
            V((nscen, nbus), F32),
            V((nscen, nline), I32),
            V((nscen, nline), F32),
            V((nscen, nline), F32),
            V((2, LANES), F32),
            V((ranks, 2, LANES), F32),
            V((planes // ranks, ranks, 2, ranks, LANES), F32),
            V((2,) + deep, I32),
            V((4,) + deep, F32),
            V((2,) + bus, F32),
            V((2,) + bus, F32),
            V((2,) + bus, F32),
            V(bus, F32),
            V(line, I32),
            V(line, F32),
            V(bus, F32),
            V((2 * nbus // LANES * ranks, 2 * LANES), BF16),
            V((8,) + deep, F32),
            V((6,) + deep, F32),
            V((240, 256), F32),
            V((2,) + bus, F32),
            V(bus, F32),
            V(line, F32),
            V((1, LANES), F32),
            V((ranks, 1, LANES), F32),
            V((1, LANES), F32),
            V((planes, 1, LANES), F32),
            sem((13,)),
            sem((13,)),
            sem((13,)),
            sem((2,)),
            sem((2,)),
            sem,
            sem,
            sem,
            sem,
        ],
        compiler_params=pltpu.CompilerParams(collective_id=0, has_side_effects=True),
        name="residuals",
    )(
        row(base_vm),
        row(base_va),
        grid(from_bus),
        grid(to_bus),
        grid(conduct),
        grid(suscept),
        grid(charging),
        grid(rating),
        delta_state,
        multipliers,
        net_inj,
        ang_grad,
        status,
        slack,
        zdual,
    )
    mis, dual, limit, norms, total = (pltpu.with_memory_space_constraint(r, V) for r in results)
    norms, total, mis, dual, limit = pl.pallas_call(
        hand_out,
        out_shape=(
            jax.ShapeDtypeStruct((4, nscen), F32),
            jax.ShapeDtypeStruct((1, 4), F32),
            jax.ShapeDtypeStruct((nscen, 2, nbus), F32),
            jax.ShapeDtypeStruct((nscen, nbus), F32),
            jax.ShapeDtypeStruct((nscen, nline), F32),
        ),
        in_specs=[vmem] * 5,
        out_specs=(vmem, vmem, hbm, hbm, hbm),
        scratch_shapes=[sem((3,))],
        name="hand_out",
    )(norms, total, mis, dual, limit)
    return mis, dual, limit, norms.T, total.reshape(4)


def solution(mesh):
    placed = (
        P(("ctg", "br")),
        P(("ctg", "br")),
        P("ctg", None, "br"),
        P("ctg", None, "br"),
        P("ctg", None, "br"),
        P("ctg", "br"),
        P("br"),
        P("br"),
        P("ctg", "br"),
        P("br"),
        P("br"),
        P("br"),
        P("br"),
        P("ctg", "br"),
        P("ctg", "br"),
    )
    return jax.shard_map(
        per_device,
        mesh=mesh,
        in_specs=placed,
        out_specs=(P("ctg", None, "br"), P("ctg", "br"), P("ctg", "br"), P("ctg", None), P()),
        check_vma=False,
    )
```

```python
import functools

import jax
import jax.numpy as jnp
from jax import lax
from jax.experimental import pallas as pl
from jax.experimental.pallas import tpu as pltpu
from jax.sharding import PartitionSpec as P

F32, I32, BF16 = jnp.float32, jnp.int32, jnp.bfloat16
LANES = 128
MESH = pl.DeviceIdType.MESH


def kernel(
    planes,
    ranks,
    base_vm,
    base_va,
    from_bus,
    to_bus,
    conduct,
    suscept,
    charging,
    rating,
    delta,
    mult,
    net,
    ang,
    status,
    slack,
    zdual,
    mismatch,
    dual,
    limit,
    norms,
    total,
    lines_i,
    lines_f,
    delta_v,
    mult_v,
    net_v,
    ang_v,
    status_v,
    slack_v,
    zdual_v,
    base_v,
    base_z,
    base_all,
    idx,
    coef,
    mult_all,
    delta_all,
    net_all,
    ang_all,
    status_all,
    slack_all,
    angles,
    stacked,
    ends,
    terms,
    sums,
    mis_out,
    dual_out,
    limit_out,
    sq_mine,
    sq_all,
    tot_mine,
    tot_all,
    load_sem,
    send_sem,
    recv_sem,
    pass_send,
    pass_recv,
    base_send,
    base_recv,
    tot_send,
    tot_recv,
):
    me = lax.axis_index("ctg")
    rank = lax.axis_index("br")
    core = lax.rem(me, 2)
    partner = me + 1 - 2 * core
    nbus = delta.shape[2]
    nline = status.shape[1]
    bus_tiles, line_tiles = nbus // LANES, nline // LANES

    pairs = (
        (from_bus, lines_i.at[0]),
        (to_bus, lines_i.at[1]),
        (mult, mult_v),
        (delta, delta_v),
        (conduct, lines_f.at[0]),
        (suscept, lines_f.at[1]),
        (charging, lines_f.at[2]),
        (rating, lines_f.at[3]),
        (status, status_v),
        (slack, slack_v),
        (net, net_v),
        (ang, ang_v),
        (zdual, zdual_v),
    )
    loads = [pltpu.make_async_copy(a, b, load_sem.at[n]) for n, (a, b) in enumerate(pairs)]
    for c in loads:
        c.start()

    barrier = pltpu.get_barrier_semaphore()
    for d in range(1, ranks):
        pl.semaphore_signal(barrier, 1, device_id=(me, lax.rem(rank + d, ranks)), device_id_type=MESH)

    def greet(d, carry):
        pl.semaphore_signal(barrier, 1, device_id=(lax.rem(me + d, planes), rank), device_id_type=MESH)
        return carry

    lax.fori_loop(1, planes, greet, 0)
    piece = base_vm.shape[1]
    base_v[0:1, 0:piece] = base_vm[...]
    base_v[1:2, 0:piece] = base_va[...]
    for c in loads:
        c.wait()

    lane8 = lax.broadcasted_iota(I32, (ranks, LANES), 1)
    row8 = lax.broadcasted_iota(I32, (ranks, LANES), 0)
    comp_sq = jnp.zeros((ranks, LANES), F32)
    for t in range(line_tiles):
        cols = slice(t * LANES, (t + 1) * LANES)
        comp = status_v[:, cols].astype(F32) * (zdual_v[:, cols] * slack_v[:, cols] - 0.01)
        comp_sq += comp * comp
    comp_sum = jnp.sum(comp_sq, axis=1, keepdims=True)
    comp_row = jnp.sum(jnp.where(lane8 == row8 + 8, comp_sum, 0.0), axis=0, keepdims=True)

    pl.semaphore_wait(barrier, ranks - 1 + planes - 1)

    half = lambda ref: ref.at[pl.ds(2 * core, 2)]
    groups = (
        (lambda s: base_v, lambda r: base_z.at[r], base_z),
        (lambda s: lines_i.at[core], lambda r: idx.at[core, :, r, :], idx.at[core]),
        (lambda s: mult_v.at[s], lambda r: mult_all.at[:, r, :], mult_all),
        (lambda s: delta_v.at[s], lambda r: delta_all.at[:, r, :], delta_all),
        (lambda s: half(lines_f), lambda r: coef.at[pl.ds(2 * core, 2), :, r, :], half(coef)),
        (lambda s: status_v.at[s], lambda r: status_all.at[r], status_all),
        (lambda s: slack_v.at[s], lambda r: slack_all.at[r], slack_all),
        (lambda s: net_v.at[s], lambda r: net_all.at[:, r, :], net_all),
        (lambda s: ang_v.at[s], lambda r: ang_all.at[r], ang_all),
    )

    def send(n, source, place):
        pltpu.make_async_copy(source(rank), place(rank), recv_sem.at[n]).start()
        for d in range(1, ranks):
            peer = lax.rem(rank + d, ranks)
            pltpu.make_async_remote_copy(
                src_ref=source(peer),
                dst_ref=place(rank),
                send_sem=send_sem.at[n],
                recv_sem=recv_sem.at[n],
                device_id=(me, peer),
                device_id_type=MESH,
            ).start()

    def take(n, whole):
        pltpu.make_async_copy(whole, whole, recv_sem.at[n]).wait()

    for n, (source, place, _) in enumerate(groups):
        send(n, source, place)

    def across(n, mine, theirs):
        out = pltpu.make_async_remote_copy(
            src_ref=mine,
            dst_ref=mine,
            send_sem=pass_send.at[n],
            recv_sem=pass_recv.at[n],
            device_id=(partner, rank),
            device_id_type=MESH,
        )
        out.start()
        return out, pltpu.make_async_copy(theirs, theirs, pass_recv.at[n])

    take(0, base_z)
    group = planes // ranks
    home = base_all.at[lax.rem(me, group), :, :, me // group, :]
    pltpu.make_async_copy(base_z, home, base_recv).start()

    def spread(d, carry):
        pltpu.make_async_remote_copy(
            src_ref=base_z,
            dst_ref=home,
            send_sem=base_send,
            recv_sem=base_recv,
            device_id=(lax.rem(me + d, planes), rank),
            device_id_type=MESH,
        ).start()
        return carry

    lax.fori_loop(1, planes, spread, 0)

    take(1, idx.at[core])
    idx_out, idx_in = across(0, idx.at[core], idx.at[1 - core])
    take(2, mult_all)
    idx_in.wait()

    row16 = lax.broadcasted_iota(I32, (16, LANES), 0)
    ramp16 = row16.astype(F32).astype(BF16)
    none16, one16 = jnp.zeros((16, LANES), BF16), jnp.ones((16, LANES), BF16)
    high_row = [row8 * bus_tiles + t for t in range(bus_tiles)]
    n_rows = ranks * bus_tiles

    def one_hot(low, tiles):
        low = jnp.broadcast_to(low.astype(F32), (16, LANES)).astype(BF16)
        return jnp.concatenate(
            [jnp.where(low == ramp16 + BF16(16 * t), one16, none16) for t in range(tiles)], 0
        )

    def stack(q, tile):
        for t in range(0, bus_tiles, 2):
            both = jnp.concatenate([tile(t), tile(t + 1)], 0)
            coarse = both.astype(BF16)
            rows = slice(q * n_rows + ranks * t, q * n_rows + ranks * (t + 2))
            stacked[rows, 0:LANES] = coarse
            stacked[rows, LANES:] = (both - coarse.astype(F32)).astype(BF16)

    def by_matmul(k, count, store):
        for e in range(2):
            out = [jnp.zeros((ranks, LANES), F32) for _ in range(count)]
            for s in range(0, ranks, 2):
                hot, high = [], []
                for n in range(2):
                    bus = idx[e, k, s + n : s + n + 1, :]
                    high.append(jnp.broadcast_to(bus >> 7, (ranks, LANES)))
                    hot.append(one_hot(bus & 127, LANES // 16))
                hot = jnp.concatenate(hot, 1)
                rows = jnp.dot(
                    stacked[0 : count * n_rows, :],
                    jnp.concatenate([hot, hot], 0),
                    preferred_element_type=F32,
                )
                for n in range(2):
                    for q in range(count):
                        acc = jnp.zeros((ranks, LANES), F32)
                        for t in range(bus_tiles):
                            first = q * n_rows + ranks * t
                            part = rows[first : first + ranks, n * LANES : (n + 1) * LANES]
                            acc = jnp.where(high[n] == high_row[t], part, acc)
                        for step in (4, 2, 1):
                            acc = acc + pltpu.roll(acc, step, 0)
                        out[q] = jnp.where(row8 == s + n, acc, out[q])
            for q in range(count):
                store(e, q, out[q])

    def by_permute(k, store):
        for e in range(2):
            bus = idx[e, k]
            high, low = bus >> 7, bus & 127
            found = jnp.zeros((ranks, LANES), F32)
            for h in range(n_rows):
                r, t = h // bus_tiles, h % bus_tiles
                row = jnp.broadcast_to(angles[r : r + 1, t * LANES : (t + 1) * LANES], (ranks, LANES))
                got = jnp.take_along_axis(row, low, axis=1, mode="promise_in_bounds")
                found = jnp.where(high == h, got, found)
            store(e, found)

    for q in range(2):
        stack(q, lambda t: mult_all[q, :, t * LANES : (t + 1) * LANES])

    def gather_mult(k, carry):
        def store(e, q, value):
            ends[4 * e + 2 + q, k] = value

        by_matmul(k, 2, store)
        return carry

    lax.fori_loop(0, line_tiles, gather_mult, 0, unroll=True)

    take(3, delta_all)
    pltpu.make_async_copy(base_all, base_all, base_recv).wait()
    for q in range(2):
        tiles = [jnp.zeros((ranks, LANES), F32) for _ in range(bus_tiles)]
        for p in range(nbus // piece):
            rows = base_all[p // ranks, p % ranks, q]
            t, off = p * piece // LANES, p * piece % LANES
            moved = pltpu.roll(rows, off, 1) if off else rows
            tiles[t] = jnp.where((lane8 >= off) & (lane8 < off + piece), moved, tiles[t])
            if off + piece > LANES:
                tiles[t + 1] = jnp.where(lane8 < off + piece - LANES, moved, tiles[t + 1])
        for t in range(bus_tiles):
            cols = slice(t * LANES, (t + 1) * LANES)
            tiles[t] = tiles[t] + delta_all[q, :, cols]
            if q == 1:
                angles[:, cols] = tiles[t]
        if q == 0:
            stack(0, lambda t: tiles[t] - 1.0)

    take(4, half(coef))
    coef_out, coef_in = across(1, half(coef), coef.at[pl.ds(2 - 2 * core, 2)])

    def gather_volt(k, carry):
        def store_vm(e, q, value):
            ends[4 * e, k] = value + 1.0

        def store_va(e, value):
            ends[4 * e + 1, k] = value

        by_permute(k, store_va)
        by_matmul(k, 1, store_vm)
        return carry

    lax.fori_loop(0, line_tiles, gather_volt, 0, unroll=True)

    coef_in.wait()
    take(5, status_all)

    def flows(k, carry):
        cols = pl.ds(pl.multiple_of(k * LANES, LANES), LANES)
        vf, af, mpf, mqf = (ends[q, k] for q in range(4))
        vt, at, mpt, mqt = (ends[4 + q, k] for q in range(4))
        g, b, h = (coef[q, k] for q in range(3))
        live = status_all[:, cols].astype(F32)
        diff = af - at
        cs, sn = jnp.cos(diff), jnp.sin(diff)
        u = vf * vt
        gcs, gsn, bcs, bsn = g * cs, g * sn, b * cs, b * sn
        pf = (g * vf * vf - u * (gcs + bsn)) * live
        qf = (-(b + h) * vf * vf - u * (gsn - bcs)) * live
        pt = (g * vt * vt - u * (gcs - bsn)) * live
        qt = (-(b + h) * vt * vt + u * (gsn + bcs)) * live
        fd = u * (mpf * (gsn - bcs) - mqf * (gcs + bsn) + mpt * (gsn + bcs) + mqt * (gcs - bsn)) * live
        for n, v in enumerate((pf, qf, fd, pt, qt, -fd)):
            terms[n, k] = v
        return carry

    lax.fori_loop(0, line_tiles, flows, 0, unroll=True)

    take(6, slack_all)
    limit_sq = jnp.zeros((ranks, LANES), F32)
    for k in range(line_tiles):
        cols = slice(k * LANES, (k + 1) * LANES)
        pf, qf = terms[0, k], terms[1, k]
        live = status_all[:, cols].astype(F32)
        lim = live * (pf * pf + qf * qf + slack_all[:, cols] - coef[3, k] * coef[3, k])
        limit_out[:, cols] = lim
        limit_sq += lim * lim

    n_limit, n_mis, n_dual, n_sq = (len(groups) + n for n in range(4))
    send(n_limit, lambda s: limit_out.at[s], lambda r: limit.at[r])

    per = nbus // 256
    high_of = [((row16 & 7) * per + j).astype(F32).astype(BF16) for j in range(per)]
    sums[...] = jnp.zeros_like(sums)

    def scatter(k, carry):
        for s in range(ranks):
            left, right = [], []
            for e in range(2):
                at_bus = idx[e, k, s : s + 1, :]
                high = jnp.broadcast_to((at_bus >> 8).astype(F32), (16, LANES)).astype(BF16)
                vals = []
                for r in range(3):
                    v = terms[3 * e + r, k, s : s + 1, :]
                    coarse = v.astype(BF16).astype(F32)
                    fine = v - coarse
                    vals.append(
                        jnp.concatenate(
                            [jnp.broadcast_to(coarse, (8, LANES)), jnp.broadcast_to(fine, (8, LANES))], 0
                        ).astype(BF16)
                    )
                rows = []
                for j in range(per):
                    here = high == high_of[j]
                    rows += [jnp.where(here, v, none16) for v in vals]
                left.append(jnp.concatenate(rows, 0))
                right.append(one_hot(at_bus & 255, 16))
            sums[...] += lax.dot_general(
                jnp.concatenate(left, 1),
                jnp.concatenate(right, 1),
                (((1,), (1,)), ((), ())),
                preferred_element_type=F32,
            )
        return carry

    lax.fori_loop(0, line_tiles, scatter, 0, unroll=True)

    take(7, net_all)
    take(8, ang_all)
    mis_sq, dual_sq = jnp.zeros((ranks, 256), F32), jnp.zeros((ranks, 256), F32)
    for j in range(per):
        cols = slice(256 * j, 256 * (j + 1))
        for r in range(3):
            first = (3 * j + r) * 16
            got = sums[first : first + 8, :] + sums[first + 8 : first + 16, :]
            if r < 2:
                out = got - net_all[r, :, cols]
                mis_out[r, :, cols] = out
                mis_sq += out * out
            else:
                out = got + ang_all[:, cols]
                dual_out[:, cols] = out
                dual_sq += out * out

    mine = comp_row
    for n, part in enumerate((mis_sq, dual_sq, limit_sq)):
        mine = jnp.where(lane8[0:1] == n, jnp.sum(part, keepdims=True), mine)
    sq_mine[...] = mine
    send(n_sq, lambda s: sq_mine, lambda r: sq_all.at[r])
    send(n_mis, lambda s: mis_out.at[:, s, :], lambda r: mismatch.at[r])
    send(n_dual, lambda s: dual_out.at[s], lambda r: dual.at[r])

    take(n_sq, sq_all)
    every = sq_all[:, 0, :]
    comp_all = jnp.sum(every, axis=0, keepdims=True)
    comp_of = jnp.sum(jnp.where(lane8 == row8 + 8, comp_all, 0.0), axis=1, keepdims=True)
    squares = jnp.where(lane8 == 3, comp_of, jnp.where(lane8 < 3, every, 0.0))
    tot_mine[...] = jnp.sum(squares, axis=0, keepdims=True)
    pltpu.make_async_copy(tot_mine, tot_all.at[me], tot_recv).start()

    def share(d, carry):
        pltpu.make_async_remote_copy(
            src_ref=tot_mine,
            dst_ref=tot_all.at[me],
            send_sem=tot_send,
            recv_sem=tot_recv,
            device_id=(lax.rem(me + d, planes), rank),
            device_id_type=MESH,
        ).start()
        return carry

    lax.fori_loop(1, planes, share, 0)
    norms[...] = jnp.sqrt(squares)
    take(n_limit, limit)
    take(n_mis, mismatch)
    take(n_dual, dual)
    idx_out.wait_send()
    coef_out.wait_send()
    for n, (_, _, dest) in enumerate(groups):
        sent(send_sem.at[n], dest, ranks)
    for n, dest in ((n_limit, limit), (n_mis, mismatch), (n_dual, dual), (n_sq, sq_all)):
        sent(send_sem.at[n], dest, ranks)
    part = base_all.at[:, :, :, 0 : ranks - 1, :]
    pltpu.make_async_copy(part, part, base_send).wait()
    part = base_all.at[0 : group - 1, :, :, ranks - 1, :]
    pltpu.make_async_copy(part, part, base_send).wait()
    pltpu.make_async_copy(tot_all, tot_all, tot_recv).wait()
    whole = jnp.sum(tot_all[:, 0, :], axis=0, keepdims=True)
    total[...] = jnp.sqrt(whole / (planes * ranks))
    part = tot_all.at[0 : planes - 1]
    pltpu.make_async_copy(part, part, tot_send).wait()


def sent(sem, dest, ranks):
    dim = len(dest.shape) - 1 - dest.shape[::-1].index(ranks)
    part = dest.at[(slice(None),) * dim + (slice(0, ranks - 1),)]
    pltpu.make_async_copy(part, part, sem).wait()


def hand_out(norms, total, mis, dual, limit, norms_out, total_out, mis_out, dual_out, limit_out, sem):
    pairs = ((mis, mis_out), (dual, dual_out), (limit, limit_out))
    copies = [pltpu.make_async_copy(a, b, sem.at[n]) for n, (a, b) in enumerate(pairs)]
    for c in copies:
        c.start()
    norms_out[...] = norms[...].T[0:4, :]
    total_out[...] = total[:, 0:4]
    for c in copies:
        c.wait()


def per_device(
    base_vm,
    base_va,
    delta_state,
    multipliers,
    net_inj,
    ang_grad,
    from_bus,
    to_bus,
    status,
    conduct,
    suscept,
    charging,
    rating,
    slack,
    zdual,
):
    planes, ranks = lax.axis_size("ctg"), lax.axis_size("br")
    nscen, _, nbus = delta_state.shape
    nline = status.shape[1]
    tiles = nline // LANES
    hbm = pl.BlockSpec(memory_space=pl.ANY)
    vmem = pl.BlockSpec(memory_space=pltpu.VMEM)
    V = pltpu.VMEM
    bus, line, deep = (ranks, nbus), (ranks, nline), (tiles, ranks, LANES)
    sem = pltpu.SemaphoreType.DMA
    row = lambda a: a.reshape(1, -1)
    grid = lambda a: a.reshape(tiles, LANES)
    results = pl.pallas_call(
        functools.partial(kernel, planes, ranks),
        out_shape=(
            V((nscen, 2, nbus), F32),
            V((nscen, nbus), F32),
            V((nscen, nline), F32),
            V((nscen, LANES), F32),
            V((1, LANES), F32),
        ),
        in_specs=[vmem] * 2 + [hbm] * 13,
        out_specs=(vmem,) * 5,
        scratch_shapes=[
            V((2, tiles, LANES), I32),
            V((4, tiles, LANES), F32),
            V((nscen, 2, nbus), F32),
            V((nscen, 2, nbus), F32),
            V((nscen, 2, nbus), F32),
            V((nscen, nbus), F32),
            V((nscen, nline), I32),
            V((nscen, nline), F32),
            V((nscen, nline), F32),
            V((2, LANES), F32),
            V((ranks, 2, LANES), F32),
            V((planes // ranks, ranks, 2, ranks, LANES), F32),
            V((2,) + deep, I32),
            V((4,) + deep, F32),
            V((2,) + bus, F32),
            V((2,) + bus, F32),
            V((2,) + bus, F32),
            V(bus, F32),
            V(line, I32),
            V(line, F32),
            V(bus, F32),
            V((2 * nbus // LANES * ranks, 2 * LANES), BF16),
            V((8,) + deep, F32),
            V((6,) + deep, F32),
            V((240, 256), F32),
            V((2,) + bus, F32),
            V(bus, F32),
            V(line, F32),
            V((1, LANES), F32),
            V((ranks, 1, LANES), F32),
            V((1, LANES), F32),
            V((planes, 1, LANES), F32),
            sem((13,)),
            sem((13,)),
            sem((13,)),
            sem((2,)),
            sem((2,)),
            sem,
            sem,
            sem,
            sem,
        ],
        compiler_params=pltpu.CompilerParams(collective_id=0, has_side_effects=True),
        name="residuals",
    )(
        row(base_vm),
        row(base_va),
        grid(from_bus),
        grid(to_bus),
        grid(conduct),
        grid(suscept),
        grid(charging),
        grid(rating),
        delta_state,
        multipliers,
        net_inj,
        ang_grad,
        status,
        slack,
        zdual,
    )
    mis, dual, limit, norms, total = (pltpu.with_memory_space_constraint(r, V) for r in results)
    norms, total, mis, dual, limit = pl.pallas_call(
        hand_out,
        out_shape=(
            jax.ShapeDtypeStruct((4, nscen), F32),
            jax.ShapeDtypeStruct((1, 4), F32),
            jax.ShapeDtypeStruct((nscen, 2, nbus), F32),
            jax.ShapeDtypeStruct((nscen, nbus), F32),
            jax.ShapeDtypeStruct((nscen, nline), F32),
        ),
        in_specs=[vmem] * 5,
        out_specs=(vmem, vmem, hbm, hbm, hbm),
        scratch_shapes=[sem((3,))],
        name="hand_out",
    )(norms, total, mis, dual, limit)
    return mis, dual, limit, norms.T, total.reshape(4)


def solution(mesh):
    placed = (
        P(("ctg", "br")),
        P(("ctg", "br")),
        P("ctg", None, "br"),
        P("ctg", None, "br"),
        P("ctg", None, "br"),
        P("ctg", "br"),
        P("br"),
        P("br"),
        P("ctg", "br"),
        P("br"),
        P("br"),
        P("br"),
        P("br"),
        P("ctg", "br"),
        P("ctg", "br"),
    )
    return jax.shard_map(
        per_device,
        mesh=mesh,
        in_specs=placed,
        out_specs=(P("ctg", None, "br"), P("ctg", "br"), P("ctg", "br"), P("ctg", None), P()),
        check_vma=False,
    )
```

```python
import functools

import jax
import jax.numpy as jnp
from jax import lax
from jax.experimental import pallas as pl
from jax.experimental.pallas import tpu as pltpu
from jax.sharding import PartitionSpec as P

F32, I32, BF16 = jnp.float32, jnp.int32, jnp.bfloat16
LANES = 128
MESH = pl.DeviceIdType.MESH


def kernel(
    planes,
    ranks,
    base_vm,
    base_va,
    from_bus,
    to_bus,
    conduct,
    suscept,
    charging,
    rating,
    delta,
    mult,
    net,
    ang,
    status,
    slack,
    zdual,
    mismatch,
    dual,
    limit,
    norms,
    total,
    lines_i,
    lines_f,
    delta_v,
    mult_v,
    net_v,
    ang_v,
    status_v,
    slack_v,
    zdual_v,
    base_s,
    base_v,
    base_z,
    base_all,
    idx,
    coef,
    mult_all,
    delta_all,
    net_all,
    ang_all,
    status_all,
    slack_all,
    angles,
    stacked,
    ends,
    terms,
    sums,
    mis_out,
    dual_out,
    limit_out,
    sq_mine,
    sq_all,
    tot_mine,
    tot_all,
    load_sem,
    send_sem,
    recv_sem,
    pass_send,
    pass_recv,
    base_send,
    base_recv,
    tot_send,
    tot_recv,
):
    me = lax.axis_index("ctg")
    rank = lax.axis_index("br")
    core = lax.rem(me, 2)
    partner = me + 1 - 2 * core
    nbus = delta.shape[2]
    nline = status.shape[1]
    bus_tiles, line_tiles = nbus // LANES, nline // LANES

    loads = {}

    def load(name, source, place):
        loads[name] = pltpu.make_async_copy(source, place, load_sem.at[len(loads)])
        loads[name].start()

    def loaded(*names):
        for name in names:
            loads[name].wait()

    load("from", from_bus, lines_i.at[0])
    load("to", to_bus, lines_i.at[1])
    load("mult", mult, mult_v)
    load("vm", base_vm, base_s.at[0])
    load("va", base_va, base_s.at[1])
    load("delta", delta, delta_v)

    barrier = pltpu.get_barrier_semaphore()
    for d in range(1, ranks):
        pl.semaphore_signal(barrier, 1, device_id=(me, lax.rem(rank + d, ranks)), device_id_type=MESH)

    def greet(d, carry):
        pl.semaphore_signal(barrier, 1, device_id=(lax.rem(me + d, planes), rank), device_id_type=MESH)
        return carry

    lax.fori_loop(1, planes, greet, 0)

    for n, ref in enumerate((conduct, suscept, charging, rating)):
        load(n, ref, lines_f.at[n])
    load("status", status, status_v)
    load("slack", slack, slack_v)
    load("net", net, net_v)
    load("ang", ang, ang_v)
    load("zdual", zdual, zdual_v)

    lane8 = lax.broadcasted_iota(I32, (ranks, LANES), 1)
    row8 = lax.broadcasted_iota(I32, (ranks, LANES), 0)
    piece = base_vm.shape[0]
    loaded("vm", "va")
    for q in range(2):
        spread_out = jnp.zeros((1, LANES), F32)
        for n in range(piece):
            spread_out = jnp.where(lane8[0:1] == n, base_s[q, n], spread_out)
        base_v[q : q + 1, :] = spread_out
    loaded("from", "to", "mult")

    pl.semaphore_wait(barrier, ranks - 1 + planes - 1)

    quad = lax.rem(me, 4)
    groups = (
        (lambda s: base_v, lambda r: base_z.at[r], base_z),
        (lambda s: lines_i.at[core], lambda r: idx.at[core, :, r, :], idx.at[core]),
        (lambda s: mult_v.at[s], lambda r: mult_all.at[:, r, :], mult_all),
        (lambda s: delta_v.at[s], lambda r: delta_all.at[:, r, :], delta_all),
        (lambda s: lines_f.at[quad], lambda r: coef.at[quad, :, r, :], coef.at[quad]),
        (lambda s: status_v.at[s], lambda r: status_all.at[r], status_all),
        (lambda s: slack_v.at[s], lambda r: slack_all.at[r], slack_all),
        (lambda s: net_v.at[s], lambda r: net_all.at[:, r, :], net_all),
        (lambda s: ang_v.at[s], lambda r: ang_all.at[r], ang_all),
    )

    def send(n, source, place):
        pltpu.make_async_copy(source(rank), place(rank), recv_sem.at[n]).start()
        for d in range(1, ranks):
            peer = lax.rem(rank + d, ranks)
            pltpu.make_async_remote_copy(
                src_ref=source(peer),
                dst_ref=place(rank),
                send_sem=send_sem.at[n],
                recv_sem=recv_sem.at[n],
                device_id=(me, peer),
                device_id_type=MESH,
            ).start()

    def take(n, whole):
        pltpu.make_async_copy(whole, whole, recv_sem.at[n]).wait()

    needs = {3: ("delta",), 4: (0, 1, 2, 3), 5: ("status",), 6: ("slack",), 7: ("net",), 8: ("ang",)}
    for n in (0, 1, 2, 4, 3, 5, 6, 7, 8):
        loaded(*needs.get(n, ()))
        send(n, *groups[n][:2])

    take(1, idx.at[core])
    idx_out = pltpu.make_async_remote_copy(
        src_ref=idx.at[core],
        dst_ref=idx.at[core],
        send_sem=pass_send.at[0],
        recv_sem=pass_recv.at[0],
        device_id=(partner, rank),
        device_id_type=MESH,
    )
    idx_out.start()
    take(0, base_z)
    group = planes // ranks
    home = base_all.at[lax.rem(me, group), :, :, me // group, :]
    pltpu.make_async_copy(base_z, home, base_recv).start()

    def spread(d, carry):
        pltpu.make_async_remote_copy(
            src_ref=base_z,
            dst_ref=home,
            send_sem=base_send,
            recv_sem=base_recv,
            device_id=(lax.rem(me + d, planes), rank),
            device_id_type=MESH,
        ).start()
        return carry

    lax.fori_loop(1, planes, spread, 0)

    loaded("zdual")
    comp_sq = jnp.zeros((ranks, LANES), F32)
    for t in range(line_tiles):
        cols = slice(t * LANES, (t + 1) * LANES)
        comp = status_v[:, cols].astype(F32) * (zdual_v[:, cols] * slack_v[:, cols] - 0.01)
        comp_sq += comp * comp
    comp_sum = jnp.sum(comp_sq, axis=1, keepdims=True)
    comp_row = jnp.sum(jnp.where(lane8 == row8 + 8, comp_sum, 0.0), axis=0, keepdims=True)

    take(2, mult_all)
    pltpu.make_async_copy(idx.at[1 - core], idx.at[1 - core], pass_recv.at[0]).wait()

    row16 = lax.broadcasted_iota(I32, (16, LANES), 0)
    ramp16 = row16.astype(F32).astype(BF16)
    none16, one16 = jnp.zeros((16, LANES), BF16), jnp.ones((16, LANES), BF16)
    high_row = [row8 * bus_tiles + t for t in range(bus_tiles)]
    n_rows = ranks * bus_tiles

    def one_hot(low, tiles):
        low = jnp.broadcast_to(low.astype(F32), (16, LANES)).astype(BF16)
        return jnp.concatenate(
            [jnp.where(low == ramp16 + BF16(16 * t), one16, none16) for t in range(tiles)], 0
        )

    def stack(q, tile):
        for t in range(0, bus_tiles, 2):
            both = jnp.concatenate([tile(t), tile(t + 1)], 0)
            coarse = both.astype(BF16)
            rows = slice(q * n_rows + ranks * t, q * n_rows + ranks * (t + 2))
            stacked[rows, 0:LANES] = coarse
            stacked[rows, LANES:] = (both - coarse.astype(F32)).astype(BF16)

    def by_matmul(k, count, store):
        for e in range(2):
            out = [jnp.zeros((ranks, LANES), F32) for _ in range(count)]
            for s in range(0, ranks, 2):
                hot, high = [], []
                for n in range(2):
                    bus = idx[e, k, s + n : s + n + 1, :]
                    high.append(jnp.broadcast_to(bus >> 7, (ranks, LANES)))
                    hot.append(one_hot(bus & 127, LANES // 16))
                hot = jnp.concatenate(hot, 1)
                rows = jnp.dot(
                    stacked[0 : count * n_rows, :],
                    jnp.concatenate([hot, hot], 0),
                    preferred_element_type=F32,
                )
                for n in range(2):
                    for q in range(count):
                        acc = jnp.zeros((ranks, LANES), F32)
                        for t in range(bus_tiles):
                            first = q * n_rows + ranks * t
                            part = rows[first : first + ranks, n * LANES : (n + 1) * LANES]
                            acc = jnp.where(high[n] == high_row[t], part, acc)
                        for step in (4, 2, 1):
                            acc = acc + pltpu.roll(acc, step, 0)
                        out[q] = jnp.where(row8 == s + n, acc, out[q])
            for q in range(count):
                store(e, q, out[q])

    def by_permute(k, store):
        for e in range(2):
            bus = idx[e, k]
            high, low = bus >> 7, bus & 127
            found = jnp.zeros((ranks, LANES), F32)
            for h in range(n_rows):
                r, t = h // bus_tiles, h % bus_tiles
                row = jnp.broadcast_to(angles[r : r + 1, t * LANES : (t + 1) * LANES], (ranks, LANES))
                got = jnp.take_along_axis(row, low, axis=1, mode="promise_in_bounds")
                found = jnp.where(high == h, got, found)
            store(e, found)

    for q in range(2):
        stack(q, lambda t: mult_all[q, :, t * LANES : (t + 1) * LANES])

    def gather_mult(k, carry):
        def store(e, q, value):
            ends[4 * e + 2 + q, k] = value

        by_matmul(k, 2, store)
        return carry

    middle = line_tiles // 3
    lax.fori_loop(0, middle, gather_mult, 0, unroll=True)
    take(4, coef.at[quad])
    for d in range(1, 4):
        pltpu.make_async_remote_copy(
            src_ref=coef.at[quad],
            dst_ref=coef.at[quad],
            send_sem=pass_send.at[1],
            recv_sem=pass_recv.at[1],
            device_id=(me - quad + lax.rem(quad + d, 4), rank),
            device_id_type=MESH,
        ).start()
    lax.fori_loop(middle, line_tiles, gather_mult, 0, unroll=True)

    take(3, delta_all)
    pltpu.make_async_copy(base_all, base_all, base_recv).wait()
    for q in range(2):
        tiles = [jnp.zeros((ranks, LANES), F32) for _ in range(bus_tiles)]
        for p in range(nbus // piece):
            rows = base_all[p // ranks, p % ranks, q]
            t, off = p * piece // LANES, p * piece % LANES
            moved = pltpu.roll(rows, off, 1) if off else rows
            tiles[t] = jnp.where((lane8 >= off) & (lane8 < off + piece), moved, tiles[t])
            if off + piece > LANES:
                tiles[t + 1] = jnp.where(lane8 < off + piece - LANES, moved, tiles[t + 1])
        for t in range(bus_tiles):
            cols = slice(t * LANES, (t + 1) * LANES)
            tiles[t] = tiles[t] + delta_all[q, :, cols]
            if q == 1:
                angles[:, cols] = tiles[t]
        if q == 0:
            stack(0, lambda t: tiles[t] - 1.0)

    def gather_volt(k, carry):
        def store_vm(e, q, value):
            ends[4 * e, k] = value + 1.0

        def store_va(e, value):
            ends[4 * e + 1, k] = value

        by_permute(k, store_va)
        by_matmul(k, 1, store_vm)
        return carry

    lax.fori_loop(0, line_tiles, gather_volt, 0, unroll=True)

    pltpu.make_async_copy(coef.at[0:3], coef.at[0:3], pass_recv.at[1]).wait()
    take(5, status_all)

    def flows(k, carry):
        cols = pl.ds(pl.multiple_of(k * LANES, LANES), LANES)
        vf, af, mpf, mqf = (ends[q, k] for q in range(4))
        vt, at, mpt, mqt = (ends[4 + q, k] for q in range(4))
        g, b, h = (coef[q, k] for q in range(3))
        live = status_all[:, cols].astype(F32)
        diff = af - at
        cs, sn = jnp.cos(diff), jnp.sin(diff)
        u = vf * vt
        gcs, gsn, bcs, bsn = g * cs, g * sn, b * cs, b * sn
        pf = (g * vf * vf - u * (gcs + bsn)) * live
        qf = (-(b + h) * vf * vf - u * (gsn - bcs)) * live
        pt = (g * vt * vt - u * (gcs - bsn)) * live
        qt = (-(b + h) * vt * vt + u * (gsn + bcs)) * live
        fd = u * (mpf * (gsn - bcs) - mqf * (gcs + bsn) + mpt * (gsn + bcs) + mqt * (gcs - bsn)) * live
        for n, v in enumerate((pf, qf, fd, pt, qt, -fd)):
            terms[n, k] = v
        return carry

    lax.fori_loop(0, line_tiles, flows, 0, unroll=True)

    take(6, slack_all)
    limit_sq = jnp.zeros((ranks, LANES), F32)
    for k in range(line_tiles):
        cols = slice(k * LANES, (k + 1) * LANES)
        pf, qf = terms[0, k], terms[1, k]
        live = status_all[:, cols].astype(F32)
        lim = live * (pf * pf + qf * qf + slack_all[:, cols] - coef[3, k] * coef[3, k])
        limit_out[:, cols] = lim
        limit_sq += lim * lim

    n_limit, n_mis, n_dual, n_sq = (len(groups) + n for n in range(4))
    send(n_limit, lambda s: limit_out.at[s], lambda r: limit.at[r])

    per = nbus // 256
    high_of = [((row16 & 7) * per + j).astype(F32).astype(BF16) for j in range(per)]
    sums[...] = jnp.zeros_like(sums)

    def scatter(k, carry):
        for s in range(ranks):
            left, right = [], []
            for e in range(2):
                at_bus = idx[e, k, s : s + 1, :]
                high = jnp.broadcast_to((at_bus >> 8).astype(F32), (16, LANES)).astype(BF16)
                vals = []
                for r in range(3):
                    v = terms[3 * e + r, k, s : s + 1, :]
                    coarse = v.astype(BF16).astype(F32)
                    fine = v - coarse
                    vals.append(
                        jnp.concatenate(
                            [jnp.broadcast_to(coarse, (8, LANES)), jnp.broadcast_to(fine, (8, LANES))], 0
                        ).astype(BF16)
                    )
                rows = []
                for j in range(per):
                    here = high == high_of[j]
                    rows += [jnp.where(here, v, none16) for v in vals]
                left.append(jnp.concatenate(rows, 0))
                right.append(one_hot(at_bus & 255, 16))
            sums[...] += lax.dot_general(
                jnp.concatenate(left, 1),
                jnp.concatenate(right, 1),
                (((1,), (1,)), ((), ())),
                preferred_element_type=F32,
            )
        return carry

    lax.fori_loop(0, line_tiles, scatter, 0, unroll=True)

    take(7, net_all)
    take(8, ang_all)
    mis_sq, dual_sq = jnp.zeros((ranks, 256), F32), jnp.zeros((ranks, 256), F32)
    for j in range(per):
        cols = slice(256 * j, 256 * (j + 1))
        for r in range(3):
            first = (3 * j + r) * 16
            got = sums[first : first + 8, :] + sums[first + 8 : first + 16, :]
            if r < 2:
                out = got - net_all[r, :, cols]
                mis_out[r, :, cols] = out
                mis_sq += out * out
            else:
                out = got + ang_all[:, cols]
                dual_out[:, cols] = out
                dual_sq += out * out

    mine = comp_row
    for n, part in enumerate((mis_sq, dual_sq, limit_sq)):
        mine = jnp.where(lane8[0:1] == n, jnp.sum(part, keepdims=True), mine)
    sq_mine[...] = mine
    send(n_sq, lambda s: sq_mine, lambda r: sq_all.at[r])
    send(n_mis, lambda s: mis_out.at[:, s, :], lambda r: mismatch.at[r])
    send(n_dual, lambda s: dual_out.at[s], lambda r: dual.at[r])

    take(n_sq, sq_all)
    every = sq_all[:, 0, :]
    comp_all = jnp.sum(every, axis=0, keepdims=True)
    comp_of = jnp.sum(jnp.where(lane8 == row8 + 8, comp_all, 0.0), axis=1, keepdims=True)
    squares = jnp.where(lane8 == 3, comp_of, jnp.where(lane8 < 3, every, 0.0))
    tot_mine[...] = jnp.sum(squares, axis=0, keepdims=True)
    pltpu.make_async_copy(tot_mine, tot_all.at[me], tot_recv).start()

    def share(d, carry):
        pltpu.make_async_remote_copy(
            src_ref=tot_mine,
            dst_ref=tot_all.at[me],
            send_sem=tot_send,
            recv_sem=tot_recv,
            device_id=(lax.rem(me + d, planes), rank),
            device_id_type=MESH,
        ).start()
        return carry

    lax.fori_loop(1, planes, share, 0)
    norms[...] = jnp.sqrt(squares)
    take(n_limit, limit)
    take(n_mis, mismatch)
    take(n_dual, dual)
    idx_out.wait_send()
    pltpu.make_async_copy(coef.at[0:3], coef.at[0:3], pass_send.at[1]).wait()
    for n, (_, _, dest) in enumerate(groups):
        sent(send_sem.at[n], dest, ranks)
    for n, dest in ((n_limit, limit), (n_mis, mismatch), (n_dual, dual), (n_sq, sq_all)):
        sent(send_sem.at[n], dest, ranks)
    part = base_all.at[:, :, :, 0 : ranks - 1, :]
    pltpu.make_async_copy(part, part, base_send).wait()
    part = base_all.at[0 : group - 1, :, :, ranks - 1, :]
    pltpu.make_async_copy(part, part, base_send).wait()
    pltpu.make_async_copy(tot_all, tot_all, tot_recv).wait()
    whole = jnp.sum(tot_all[:, 0, :], axis=0, keepdims=True)
    total[...] = jnp.sqrt(whole / (planes * ranks))
    part = tot_all.at[0 : planes - 1]
    pltpu.make_async_copy(part, part, tot_send).wait()


def sent(sem, dest, ranks):
    dim = len(dest.shape) - 1 - dest.shape[::-1].index(ranks)
    part = dest.at[(slice(None),) * dim + (slice(0, ranks - 1),)]
    pltpu.make_async_copy(part, part, sem).wait()


def hand_out(norms, total, mis, dual, limit, norms_out, total_out, mis_out, dual_out, limit_out, sem):
    pairs = ((mis, mis_out), (dual, dual_out), (limit, limit_out))
    copies = [pltpu.make_async_copy(a, b, sem.at[n]) for n, (a, b) in enumerate(pairs)]
    for c in copies:
        c.start()
    norms_out[...] = norms[...].T[0:4, :]
    total_out[...] = total[:, 0:4]
    for c in copies:
        c.wait()


def per_device(
    base_vm,
    base_va,
    delta_state,
    multipliers,
    net_inj,
    ang_grad,
    from_bus,
    to_bus,
    status,
    conduct,
    suscept,
    charging,
    rating,
    slack,
    zdual,
):
    planes, ranks = lax.axis_size("ctg"), lax.axis_size("br")
    nscen, _, nbus = delta_state.shape
    nline = status.shape[1]
    tiles = nline // LANES
    hbm = pl.BlockSpec(memory_space=pl.ANY)
    vmem = pl.BlockSpec(memory_space=pltpu.VMEM)
    V = pltpu.VMEM
    bus, line, deep = (ranks, nbus), (ranks, nline), (tiles, ranks, LANES)
    sem = pltpu.SemaphoreType.DMA
    grid = lambda a: a.reshape(tiles, LANES)
    results = pl.pallas_call(
        functools.partial(kernel, planes, ranks),
        out_shape=(
            V((nscen, 2, nbus), F32),
            V((nscen, nbus), F32),
            V((nscen, nline), F32),
            V((nscen, LANES), F32),
            V((1, LANES), F32),
        ),
        in_specs=[hbm] * 15,
        out_specs=(vmem,) * 5,
        scratch_shapes=[
            V((2, tiles, LANES), I32),
            V((4, tiles, LANES), F32),
            V((nscen, 2, nbus), F32),
            V((nscen, 2, nbus), F32),
            V((nscen, 2, nbus), F32),
            V((nscen, nbus), F32),
            V((nscen, nline), I32),
            V((nscen, nline), F32),
            V((nscen, nline), F32),
            pltpu.SMEM((2, base_vm.shape[0]), F32),
            V((2, LANES), F32),
            V((ranks, 2, LANES), F32),
            V((planes // ranks, ranks, 2, ranks, LANES), F32),
            V((2,) + deep, I32),
            V((4,) + deep, F32),
            V((2,) + bus, F32),
            V((2,) + bus, F32),
            V((2,) + bus, F32),
            V(bus, F32),
            V(line, I32),
            V(line, F32),
            V(bus, F32),
            V((2 * nbus // LANES * ranks, 2 * LANES), BF16),
            V((8,) + deep, F32),
            V((6,) + deep, F32),
            V((240, 256), F32),
            V((2,) + bus, F32),
            V(bus, F32),
            V(line, F32),
            V((1, LANES), F32),
            V((ranks, 1, LANES), F32),
            V((1, LANES), F32),
            V((planes, 1, LANES), F32),
            sem((15,)),
            sem((13,)),
            sem((13,)),
            sem((2,)),
            sem((2,)),
            sem,
            sem,
            sem,
            sem,
        ],
        compiler_params=pltpu.CompilerParams(collective_id=0, has_side_effects=True),
        name="residuals",
    )(
        base_vm,
        base_va,
        grid(from_bus),
        grid(to_bus),
        grid(conduct),
        grid(suscept),
        grid(charging),
        grid(rating),
        delta_state,
        multipliers,
        net_inj,
        ang_grad,
        status,
        slack,
        zdual,
    )
    mis, dual, limit, norms, total = (pltpu.with_memory_space_constraint(r, V) for r in results)
    norms, total, mis, dual, limit = pl.pallas_call(
        hand_out,
        out_shape=(
            jax.ShapeDtypeStruct((4, nscen), F32),
            jax.ShapeDtypeStruct((1, 4), F32),
            jax.ShapeDtypeStruct((nscen, 2, nbus), F32),
            jax.ShapeDtypeStruct((nscen, nbus), F32),
            jax.ShapeDtypeStruct((nscen, nline), F32),
        ),
        in_specs=[vmem] * 5,
        out_specs=(vmem, vmem, hbm, hbm, hbm),
        scratch_shapes=[sem((3,))],
        name="hand_out",
    )(norms, total, mis, dual, limit)
    return mis, dual, limit, norms.T, total.reshape(4)


def solution(mesh):
    placed = (
        P(("ctg", "br")),
        P(("ctg", "br")),
        P("ctg", None, "br"),
        P("ctg", None, "br"),
        P("ctg", None, "br"),
        P("ctg", "br"),
        P("br"),
        P("br"),
        P("ctg", "br"),
        P("br"),
        P("br"),
        P("br"),
        P("br"),
        P("ctg", "br"),
        P("ctg", "br"),
    )
    return jax.shard_map(
        per_device,
        mesh=mesh,
        in_specs=placed,
        out_specs=(P("ctg", None, "br"), P("ctg", "br"), P("ctg", "br"), P("ctg", None), P()),
        check_vma=False,
    )
```

```python
import functools

import jax
import jax.numpy as jnp
from jax import lax
from jax.experimental import pallas as pl
from jax.experimental.pallas import tpu as pltpu
from jax.sharding import PartitionSpec as P

F32, I32, BF16 = jnp.float32, jnp.int32, jnp.bfloat16
LANES = 128
MESH = pl.DeviceIdType.MESH


def kernel(
    planes,
    ranks,
    base_vm,
    base_va,
    from_bus,
    to_bus,
    conduct,
    suscept,
    charging,
    rating,
    delta,
    mult,
    net,
    ang,
    status,
    slack,
    zdual,
    mismatch,
    dual,
    limit,
    norms,
    total,
    lines_i,
    lines_f,
    delta_v,
    mult_v,
    net_v,
    ang_v,
    status_v,
    slack_v,
    zdual_v,
    base_s,
    base_v,
    base_z,
    base_all,
    idx,
    coef,
    mult_all,
    delta_all,
    net_all,
    ang_all,
    status_all,
    slack_all,
    angles,
    stacked,
    ends,
    terms,
    sums,
    mis_out,
    dual_out,
    limit_out,
    sq_mine,
    sq_all,
    tot_mine,
    tot_all,
    load_sem,
    send_sem,
    recv_sem,
    pass_send,
    pass_recv,
    base_send,
    base_recv,
    tot_send,
    tot_recv,
):
    me = lax.axis_index("ctg")
    rank = lax.axis_index("br")
    core = lax.rem(me, 2)
    partner = me + 1 - 2 * core
    nbus = delta.shape[2]
    nline = status.shape[1]
    bus_tiles, line_tiles = nbus // LANES, nline // LANES

    loads = {}

    def load(name, source, place):
        loads[name] = pltpu.make_async_copy(source, place, load_sem.at[len(loads)])
        loads[name].start()

    def loaded(*names):
        for name in names:
            loads[name].wait()

    load("from", from_bus, lines_i.at[0])
    load("to", to_bus, lines_i.at[1])
    load("mult", mult, mult_v)
    load("vm", base_vm, base_s.at[0])
    load("va", base_va, base_s.at[1])
    load("delta", delta, delta_v)

    barrier = pltpu.get_barrier_semaphore()
    for d in range(1, ranks):
        pl.semaphore_signal(barrier, 1, device_id=(me, lax.rem(rank + d, ranks)), device_id_type=MESH)

    def greet(d, carry):
        pl.semaphore_signal(barrier, 1, device_id=(lax.rem(me + d, planes), rank), device_id_type=MESH)
        return carry

    lax.fori_loop(1, planes, greet, 0)

    for n, ref in enumerate((conduct, suscept, charging, rating)):
        load(n, ref, lines_f.at[n])
    load("status", status, status_v)
    load("slack", slack, slack_v)
    load("net", net, net_v)
    load("ang", ang, ang_v)
    load("zdual", zdual, zdual_v)

    lane8 = lax.broadcasted_iota(I32, (ranks, LANES), 1)
    row8 = lax.broadcasted_iota(I32, (ranks, LANES), 0)
    piece = base_vm.shape[0]
    loaded("vm", "va")
    for q in range(2):
        spread_out = jnp.zeros((1, LANES), F32)
        for n in range(piece):
            spread_out = jnp.where(lane8[0:1] == n, base_s[q, n], spread_out)
        base_v[q : q + 1, :] = spread_out
    loaded("from", "to", "mult")

    pl.semaphore_wait(barrier, ranks - 1 + planes - 1)

    quad = lax.rem(me, 4)
    groups = (
        (lambda s: base_v, lambda r: base_z.at[r], base_z),
        (lambda s: lines_i.at[core], lambda r: idx.at[core, :, r, :], idx.at[core]),
        (lambda s: mult_v.at[s], lambda r: mult_all.at[:, r, :], mult_all),
        (lambda s: delta_v.at[s], lambda r: delta_all.at[:, r, :], delta_all),
        (lambda s: lines_f.at[quad], lambda r: coef.at[quad, :, r, :], coef.at[quad]),
        (lambda s: status_v.at[s], lambda r: status_all.at[r], status_all),
        (lambda s: slack_v.at[s], lambda r: slack_all.at[r], slack_all),
        (lambda s: net_v.at[s], lambda r: net_all.at[:, r, :], net_all),
        (lambda s: ang_v.at[s], lambda r: ang_all.at[r], ang_all),
    )

    def send(n, source, place):
        pltpu.make_async_copy(source(rank), place(rank), recv_sem.at[n]).start()
        for d in range(1, ranks):
            peer = lax.rem(rank + d, ranks)
            pltpu.make_async_remote_copy(
                src_ref=source(peer),
                dst_ref=place(rank),
                send_sem=send_sem.at[n],
                recv_sem=recv_sem.at[n],
                device_id=(me, peer),
                device_id_type=MESH,
            ).start()

    def take(n, whole):
        pltpu.make_async_copy(whole, whole, recv_sem.at[n]).wait()

    needs = {3: ("delta",), 4: (0, 1, 2, 3), 5: ("status",), 6: ("slack",), 7: ("net",), 8: ("ang",)}
    for n in (0, 1, 2, 4, 3, 5, 6, 7, 8):
        loaded(*needs.get(n, ()))
        send(n, *groups[n][:2])

    take(1, idx.at[core])
    idx_out = pltpu.make_async_remote_copy(
        src_ref=idx.at[core],
        dst_ref=idx.at[core],
        send_sem=pass_send.at[0],
        recv_sem=pass_recv.at[0],
        device_id=(partner, rank),
        device_id_type=MESH,
    )
    idx_out.start()
    take(0, base_z)
    group = planes // ranks
    home = base_all.at[lax.rem(me, group), :, :, me // group, :]
    pltpu.make_async_copy(base_z, home, base_recv).start()

    def spread(d, carry):
        pltpu.make_async_remote_copy(
            src_ref=base_z,
            dst_ref=home,
            send_sem=base_send,
            recv_sem=base_recv,
            device_id=(lax.rem(me + d, planes), rank),
            device_id_type=MESH,
        ).start()
        return carry

    lax.fori_loop(1, planes, spread, 0)

    loaded("zdual")
    comp_sq = jnp.zeros((ranks, LANES), F32)
    for t in range(line_tiles):
        cols = slice(t * LANES, (t + 1) * LANES)
        comp = status_v[:, cols].astype(F32) * (zdual_v[:, cols] * slack_v[:, cols] - 0.01)
        comp_sq += comp * comp
    comp_sum = jnp.sum(comp_sq, axis=1, keepdims=True)
    comp_row = jnp.sum(jnp.where(lane8 == row8 + 8, comp_sum, 0.0), axis=0, keepdims=True)

    take(2, mult_all)
    pltpu.make_async_copy(idx.at[1 - core], idx.at[1 - core], pass_recv.at[0]).wait()

    row16 = lax.broadcasted_iota(I32, (16, LANES), 0)
    ramp16 = row16.astype(F32).astype(BF16)
    none16, one16 = jnp.zeros((16, LANES), BF16), jnp.ones((16, LANES), BF16)
    high_row = [row8 * bus_tiles + t for t in range(bus_tiles)]
    n_rows = ranks * bus_tiles

    def one_hot(low, tiles):
        low = jnp.broadcast_to(low.astype(F32), (16, LANES)).astype(BF16)
        return jnp.concatenate(
            [jnp.where(low == ramp16 + BF16(16 * t), one16, none16) for t in range(tiles)], 0
        )

    def stack(q, tile):
        for t in range(0, bus_tiles, 2):
            both = jnp.concatenate([tile(t), tile(t + 1)], 0)
            coarse = both.astype(BF16)
            rows = slice(q * n_rows + ranks * t, q * n_rows + ranks * (t + 2))
            stacked[rows, 0:LANES] = coarse
            stacked[rows, LANES:] = (both - coarse.astype(F32)).astype(BF16)

    def by_matmul(k, count, store):
        for e in range(2):
            out = [jnp.zeros((ranks, LANES), F32) for _ in range(count)]
            for s in range(0, ranks, 2):
                hot, high = [], []
                for n in range(2):
                    bus = idx[e, k, s + n : s + n + 1, :]
                    high.append(jnp.broadcast_to(bus >> 7, (ranks, LANES)))
                    hot.append(one_hot(bus & 127, LANES // 16))
                hot = jnp.concatenate(hot, 1)
                rows = jnp.dot(
                    stacked[0 : count * n_rows, :],
                    jnp.concatenate([hot, hot], 0),
                    preferred_element_type=F32,
                )
                for n in range(2):
                    for q in range(count):
                        acc = jnp.zeros((ranks, LANES), F32)
                        for t in range(bus_tiles):
                            first = q * n_rows + ranks * t
                            part = rows[first : first + ranks, n * LANES : (n + 1) * LANES]
                            acc = jnp.where(high[n] == high_row[t], part, acc)
                        for step in (4, 2, 1):
                            acc = acc + pltpu.roll(acc, step, 0)
                        out[q] = jnp.where(row8 == s + n, acc, out[q])
            for q in range(count):
                store(e, q, out[q])

    def by_permute(k, store):
        for e in range(2):
            bus = idx[e, k]
            high, low = bus >> 7, bus & 127
            found = jnp.zeros((ranks, LANES), F32)
            for h in range(n_rows):
                r, t = h // bus_tiles, h % bus_tiles
                row = jnp.broadcast_to(angles[r : r + 1, t * LANES : (t + 1) * LANES], (ranks, LANES))
                got = jnp.take_along_axis(row, low, axis=1, mode="promise_in_bounds")
                found = jnp.where(high == h, got, found)
            store(e, found)

    for q in range(2):
        stack(q, lambda t: mult_all[q, :, t * LANES : (t + 1) * LANES])

    def gather_mult(k, carry):
        def store(e, q, value):
            ends[4 * e + 2 + q, k] = value

        by_matmul(k, 2, store)
        return carry

    middle = line_tiles // 3
    lax.fori_loop(0, middle, gather_mult, 0, unroll=True)
    take(4, coef.at[quad])
    for d in range(1, 4):
        pltpu.make_async_remote_copy(
            src_ref=coef.at[quad],
            dst_ref=coef.at[quad],
            send_sem=pass_send.at[1],
            recv_sem=pass_recv.at[1],
            device_id=(me - quad + lax.rem(quad + d, 4), rank),
            device_id_type=MESH,
        ).start()
    lax.fori_loop(middle, line_tiles, gather_mult, 0, unroll=True)

    take(3, delta_all)
    pltpu.make_async_copy(base_all, base_all, base_recv).wait()
    for q in range(2):
        tiles = [jnp.zeros((ranks, LANES), F32) for _ in range(bus_tiles)]
        for p in range(nbus // piece):
            rows = base_all[p // ranks, p % ranks, q]
            t, off = p * piece // LANES, p * piece % LANES
            moved = pltpu.roll(rows, off, 1) if off else rows
            tiles[t] = jnp.where((lane8 >= off) & (lane8 < off + piece), moved, tiles[t])
            if off + piece > LANES:
                tiles[t + 1] = jnp.where(lane8 < off + piece - LANES, moved, tiles[t + 1])
        for t in range(bus_tiles):
            cols = slice(t * LANES, (t + 1) * LANES)
            tiles[t] = tiles[t] + delta_all[q, :, cols]
            if q == 1:
                angles[:, cols] = tiles[t]
        if q == 0:
            stack(0, lambda t: tiles[t] - 1.0)

    def gather_angle(k):
        def store(e, value):
            ends[4 * e + 1, k] = value

        by_permute(k, store)

    def gather_size(k):
        def store(e, q, value):
            ends[4 * e, k] = value + 1.0

        by_matmul(k, 1, store)

    late = 4
    early = line_tiles - late

    def gather_both(k, carry):
        gather_angle(k)
        gather_size(k)
        return carry

    def gather_rest(k, carry):
        gather_size(k)
        return carry

    lax.fori_loop(0, early, gather_both, 0, unroll=True)
    lax.fori_loop(early, line_tiles, gather_rest, 0, unroll=True)

    pltpu.make_async_copy(coef.at[0:3], coef.at[0:3], pass_recv.at[1]).wait()
    take(5, status_all)

    def flows(k):
        cols = pl.ds(pl.multiple_of(k * LANES, LANES), LANES)
        vf, af, mpf, mqf = (ends[q, k] for q in range(4))
        vt, at, mpt, mqt = (ends[4 + q, k] for q in range(4))
        g, b, h = (coef[q, k] for q in range(3))
        live = status_all[:, cols].astype(F32)
        diff = af - at
        cs, sn = jnp.cos(diff), jnp.sin(diff)
        u = vf * vt
        gcs, gsn, bcs, bsn = g * cs, g * sn, b * cs, b * sn
        pf = (g * vf * vf - u * (gcs + bsn)) * live
        qf = (-(b + h) * vf * vf - u * (gsn - bcs)) * live
        pt = (g * vt * vt - u * (gcs - bsn)) * live
        qt = (-(b + h) * vt * vt + u * (gsn + bcs)) * live
        fd = u * (mpf * (gsn - bcs) - mqf * (gcs + bsn) + mpt * (gsn + bcs) + mqt * (gcs - bsn)) * live
        for n, v in enumerate((pf, qf, fd, pt, qt, -fd)):
            terms[n, k] = v

    per = nbus // 256
    high_of = [((row16 & 7) * per + j).astype(F32).astype(BF16) for j in range(per)]
    sums[...] = jnp.zeros_like(sums)

    def scatter(k):
        for s in range(ranks):
            left, right = [], []
            for e in range(2):
                at_bus = idx[e, k, s : s + 1, :]
                high = jnp.broadcast_to((at_bus >> 8).astype(F32), (16, LANES)).astype(BF16)
                vals = []
                for r in range(3):
                    v = terms[3 * e + r, k, s : s + 1, :]
                    coarse = v.astype(BF16).astype(F32)
                    fine = v - coarse
                    vals.append(
                        jnp.concatenate(
                            [jnp.broadcast_to(coarse, (8, LANES)), jnp.broadcast_to(fine, (8, LANES))], 0
                        ).astype(BF16)
                    )
                rows = []
                for j in range(per):
                    here = high == high_of[j]
                    rows += [jnp.where(here, v, none16) for v in vals]
                left.append(jnp.concatenate(rows, 0))
                right.append(one_hot(at_bus & 255, 16))
            sums[...] += lax.dot_general(
                jnp.concatenate(left, 1),
                jnp.concatenate(right, 1),
                (((1,), (1,)), ((), ())),
                preferred_element_type=F32,
            )

    def first_steps(k, carry):
        gather_angle(k + early)
        flows(k)
        scatter(k)
        return carry

    def other_steps(k, carry):
        flows(k)
        scatter(k)
        return carry

    lax.fori_loop(0, late, first_steps, 0, unroll=True)
    lax.fori_loop(late, line_tiles, other_steps, 0, unroll=True)

    take(6, slack_all)
    limit_sq = jnp.zeros((ranks, LANES), F32)
    for k in range(line_tiles):
        cols = slice(k * LANES, (k + 1) * LANES)
        pf, qf = terms[0, k], terms[1, k]
        live = status_all[:, cols].astype(F32)
        lim = live * (pf * pf + qf * qf + slack_all[:, cols] - coef[3, k] * coef[3, k])
        limit_out[:, cols] = lim
        limit_sq += lim * lim

    take(7, net_all)
    take(8, ang_all)
    mis_sq, dual_sq = jnp.zeros((ranks, 256), F32), jnp.zeros((ranks, 256), F32)
    for j in range(per):
        cols = slice(256 * j, 256 * (j + 1))
        for r in range(3):
            first = (3 * j + r) * 16
            got = sums[first : first + 8, :] + sums[first + 8 : first + 16, :]
            if r < 2:
                out = got - net_all[r, :, cols]
                mis_out[r, :, cols] = out
                mis_sq += out * out
            else:
                out = got + ang_all[:, cols]
                dual_out[:, cols] = out
                dual_sq += out * out

    mine = comp_row
    for n, part in enumerate((mis_sq, dual_sq, limit_sq)):
        mine = jnp.where(lane8[0:1] == n, jnp.sum(part, keepdims=True), mine)
    sq_mine[...] = mine
    n_limit, n_mis, n_dual, n_sq = (len(groups) + n for n in range(4))
    send(n_sq, lambda s: sq_mine, lambda r: sq_all.at[r])
    send(n_mis, lambda s: mis_out.at[:, s, :], lambda r: mismatch.at[r])
    send(n_dual, lambda s: dual_out.at[s], lambda r: dual.at[r])
    send(n_limit, lambda s: limit_out.at[s], lambda r: limit.at[r])

    take(n_sq, sq_all)
    every = sq_all[:, 0, :]
    group_sum = jnp.sum(every, axis=0, keepdims=True)
    tot_mine[...] = group_sum
    pltpu.make_async_copy(tot_mine, tot_all.at[me], tot_recv).start()

    def share(d, carry):
        pltpu.make_async_remote_copy(
            src_ref=tot_mine,
            dst_ref=tot_all.at[me],
            send_sem=tot_send,
            recv_sem=tot_recv,
            device_id=(lax.rem(me + d, planes), rank),
            device_id_type=MESH,
        ).start()
        return carry

    lax.fori_loop(1, planes, share, 0)
    comp_of = jnp.sum(jnp.where(lane8 == row8 + 8, group_sum, 0.0), axis=1, keepdims=True)
    norms[...] = jnp.sqrt(jnp.where(lane8 == 3, comp_of, jnp.where(lane8 < 3, every, 0.0)))
    take(n_limit, limit)
    take(n_mis, mismatch)
    take(n_dual, dual)
    idx_out.wait_send()
    pltpu.make_async_copy(coef.at[0:3], coef.at[0:3], pass_send.at[1]).wait()
    for n, (_, _, dest) in enumerate(groups):
        sent(send_sem.at[n], dest, ranks)
    for n, dest in ((n_limit, limit), (n_mis, mismatch), (n_dual, dual), (n_sq, sq_all)):
        sent(send_sem.at[n], dest, ranks)
    part = base_all.at[:, :, :, 0 : ranks - 1, :]
    pltpu.make_async_copy(part, part, base_send).wait()
    part = base_all.at[0 : group - 1, :, :, ranks - 1, :]
    pltpu.make_async_copy(part, part, base_send).wait()
    pltpu.make_async_copy(tot_all, tot_all, tot_recv).wait()
    whole = jnp.sum(tot_all[:, 0, :], axis=0, keepdims=True)
    lane1 = lane8[0:1]
    comp_whole = jnp.sum(jnp.where((lane1 >= 8) & (lane1 < 8 + ranks), whole, 0.0), axis=1, keepdims=True)
    whole = jnp.where(lane1 == 3, comp_whole, jnp.where(lane1 < 3, whole, 0.0))
    total[...] = jnp.sqrt(whole / (planes * ranks))
    part = tot_all.at[0 : planes - 1]
    pltpu.make_async_copy(part, part, tot_send).wait()


def sent(sem, dest, ranks):
    dim = len(dest.shape) - 1 - dest.shape[::-1].index(ranks)
    part = dest.at[(slice(None),) * dim + (slice(0, ranks - 1),)]
    pltpu.make_async_copy(part, part, sem).wait()


def hand_out(norms, total, mis, dual, limit, norms_out, total_out, mis_out, dual_out, limit_out, sem):
    pairs = ((mis, mis_out), (dual, dual_out), (limit, limit_out))
    copies = [pltpu.make_async_copy(a, b, sem.at[n]) for n, (a, b) in enumerate(pairs)]
    for c in copies:
        c.start()
    norms_out[...] = norms[...].T[0:4, :]
    total_out[...] = total[:, 0:4]
    for c in copies:
        c.wait()


def per_device(
    base_vm,
    base_va,
    delta_state,
    multipliers,
    net_inj,
    ang_grad,
    from_bus,
    to_bus,
    status,
    conduct,
    suscept,
    charging,
    rating,
    slack,
    zdual,
):
    planes, ranks = lax.axis_size("ctg"), lax.axis_size("br")
    nscen, _, nbus = delta_state.shape
    nline = status.shape[1]
    tiles = nline // LANES
    hbm = pl.BlockSpec(memory_space=pl.ANY)
    vmem = pl.BlockSpec(memory_space=pltpu.VMEM)
    V = pltpu.VMEM
    bus, line, deep = (ranks, nbus), (ranks, nline), (tiles, ranks, LANES)
    sem = pltpu.SemaphoreType.DMA
    grid = lambda a: a.reshape(tiles, LANES)
    results = pl.pallas_call(
        functools.partial(kernel, planes, ranks),
        out_shape=(
            V((nscen, 2, nbus), F32),
            V((nscen, nbus), F32),
            V((nscen, nline), F32),
            V((nscen, LANES), F32),
            V((1, LANES), F32),
        ),
        in_specs=[hbm] * 15,
        out_specs=(vmem,) * 5,
        scratch_shapes=[
            V((2, tiles, LANES), I32),
            V((4, tiles, LANES), F32),
            V((nscen, 2, nbus), F32),
            V((nscen, 2, nbus), F32),
            V((nscen, 2, nbus), F32),
            V((nscen, nbus), F32),
            V((nscen, nline), I32),
            V((nscen, nline), F32),
            V((nscen, nline), F32),
            pltpu.SMEM((2, base_vm.shape[0]), F32),
            V((2, LANES), F32),
            V((ranks, 2, LANES), F32),
            V((planes // ranks, ranks, 2, ranks, LANES), F32),
            V((2,) + deep, I32),
            V((4,) + deep, F32),
            V((2,) + bus, F32),
            V((2,) + bus, F32),
            V((2,) + bus, F32),
            V(bus, F32),
            V(line, I32),
            V(line, F32),
            V(bus, F32),
            V((2 * nbus // LANES * ranks, 2 * LANES), BF16),
            V((8,) + deep, F32),
            V((6,) + deep, F32),
            V((240, 256), F32),
            V((2,) + bus, F32),
            V(bus, F32),
            V(line, F32),
            V((1, LANES), F32),
            V((ranks, 1, LANES), F32),
            V((1, LANES), F32),
            V((planes, 1, LANES), F32),
            sem((15,)),
            sem((13,)),
            sem((13,)),
            sem((2,)),
            sem((2,)),
            sem,
            sem,
            sem,
            sem,
        ],
        compiler_params=pltpu.CompilerParams(collective_id=0, has_side_effects=True),
        name="residuals",
    )(
        base_vm,
        base_va,
        grid(from_bus),
        grid(to_bus),
        grid(conduct),
        grid(suscept),
        grid(charging),
        grid(rating),
        delta_state,
        multipliers,
        net_inj,
        ang_grad,
        status,
        slack,
        zdual,
    )
    mis, dual, limit, norms, total = (pltpu.with_memory_space_constraint(r, V) for r in results)
    norms, total, mis, dual, limit = pl.pallas_call(
        hand_out,
        out_shape=(
            jax.ShapeDtypeStruct((4, nscen), F32),
            jax.ShapeDtypeStruct((1, 4), F32),
            jax.ShapeDtypeStruct((nscen, 2, nbus), F32),
            jax.ShapeDtypeStruct((nscen, nbus), F32),
            jax.ShapeDtypeStruct((nscen, nline), F32),
        ),
        in_specs=[vmem] * 5,
        out_specs=(vmem, vmem, hbm, hbm, hbm),
        scratch_shapes=[sem((3,))],
        name="hand_out",
    )(norms, total, mis, dual, limit)
    return mis, dual, limit, norms.T, total.reshape(4)


def solution(mesh):
    placed = (
        P(("ctg", "br")),
        P(("ctg", "br")),
        P("ctg", None, "br"),
        P("ctg", None, "br"),
        P("ctg", None, "br"),
        P("ctg", "br"),
        P("br"),
        P("br"),
        P("ctg", "br"),
        P("br"),
        P("br"),
        P("br"),
        P("br"),
        P("ctg", "br"),
        P("ctg", "br"),
    )
    return jax.shard_map(
        per_device,
        mesh=mesh,
        in_specs=placed,
        out_specs=(P("ctg", None, "br"), P("ctg", "br"), P("ctg", "br"), P("ctg", None), P()),
        check_vma=False,
    )
```

```python
import functools

import jax
import jax.numpy as jnp
from jax import lax
from jax.experimental import pallas as pl
from jax.experimental.pallas import tpu as pltpu
from jax.sharding import PartitionSpec as P

F32, I32, BF16 = jnp.float32, jnp.int32, jnp.bfloat16
LANES = 128
MESH = pl.DeviceIdType.MESH


def kernel(
    planes,
    ranks,
    base_vm,
    base_va,
    from_bus,
    to_bus,
    conduct,
    suscept,
    charging,
    rating,
    delta,
    mult,
    net,
    ang,
    status,
    slack,
    zdual,
    mismatch,
    dual,
    limit,
    norms,
    total,
    lines_i,
    lines_f,
    delta_v,
    mult_v,
    net_v,
    ang_v,
    status_v,
    slack_v,
    zdual_v,
    base_s,
    base_v,
    base_z,
    base_all,
    idx,
    coef,
    mult_all,
    delta_all,
    net_all,
    ang_all,
    status_all,
    slack_all,
    angles,
    stacked,
    ends,
    terms,
    sums,
    mis_out,
    dual_out,
    limit_out,
    sq_mine,
    sq_all,
    tot_mine,
    tot_all,
    load_sem,
    send_sem,
    recv_sem,
    pass_send,
    pass_recv,
    base_send,
    base_recv,
    tot_send,
    tot_recv,
):
    me = lax.axis_index("ctg")
    rank = lax.axis_index("br")
    core = lax.rem(me, 2)
    partner = me + 1 - 2 * core
    nbus = delta.shape[2]
    nline = status.shape[1]
    bus_tiles, line_tiles = nbus // LANES, nline // LANES

    loads = {}

    def load(name, source, place):
        loads[name] = pltpu.make_async_copy(source, place, load_sem.at[len(loads)])
        loads[name].start()

    def loaded(*names):
        for name in names:
            loads[name].wait()

    load("from", from_bus, lines_i.at[0])
    load("to", to_bus, lines_i.at[1])
    load("mult", mult, mult_v)
    load("vm", base_vm, base_s.at[0])
    load("va", base_va, base_s.at[1])
    load("delta", delta, delta_v)

    barrier = pltpu.get_barrier_semaphore()
    for d in range(1, ranks):
        pl.semaphore_signal(barrier, 1, device_id=(me, lax.rem(rank + d, ranks)), device_id_type=MESH)

    def greet(d, carry):
        pl.semaphore_signal(barrier, 1, device_id=(lax.rem(me + d, planes), rank), device_id_type=MESH)
        return carry

    lax.fori_loop(1, planes, greet, 0)

    for n, ref in enumerate((conduct, suscept, charging, rating)):
        load(n, ref, lines_f.at[n])
    load("status", status, status_v)
    load("slack", slack, slack_v)
    load("net", net, net_v)
    load("ang", ang, ang_v)
    load("zdual", zdual, zdual_v)

    lane8 = lax.broadcasted_iota(I32, (ranks, LANES), 1)
    row8 = lax.broadcasted_iota(I32, (ranks, LANES), 0)
    piece = base_vm.shape[0]
    loaded("vm", "va")
    for q in range(2):
        spread_out = jnp.zeros((1, LANES), F32)
        for n in range(piece):
            spread_out = jnp.where(lane8[0:1] == n, base_s[q, n], spread_out)
        base_v[q : q + 1, :] = spread_out
    loaded("from", "to", "mult")

    pl.semaphore_wait(barrier, ranks - 1 + planes - 1)

    quad = lax.rem(me, 4)
    groups = (
        (lambda s: base_v, lambda r: base_z.at[r], base_z),
        (lambda s: lines_i.at[core], lambda r: idx.at[core, :, r, :], idx.at[core]),
        (lambda s: mult_v.at[s], lambda r: mult_all.at[:, r, :], mult_all),
        (lambda s: delta_v.at[s], lambda r: delta_all.at[:, r, :], delta_all),
        (lambda s: lines_f.at[quad], lambda r: coef.at[quad, :, r, :], coef.at[quad]),
        (lambda s: status_v.at[s], lambda r: status_all.at[r], status_all),
        (lambda s: slack_v.at[s], lambda r: slack_all.at[r], slack_all),
        (lambda s: net_v.at[s], lambda r: net_all.at[:, r, :], net_all),
        (lambda s: ang_v.at[s], lambda r: ang_all.at[r], ang_all),
    )

    def send(n, source, place):
        pltpu.make_async_copy(source(rank), place(rank), recv_sem.at[n]).start()
        for d in (4, 3, 5, 2, 6, 1, 7):
            peer = lax.rem(rank + d, ranks)
            pltpu.make_async_remote_copy(
                src_ref=source(peer),
                dst_ref=place(rank),
                send_sem=send_sem.at[n],
                recv_sem=recv_sem.at[n],
                device_id=(me, peer),
                device_id_type=MESH,
            ).start()

    def take(n, whole):
        pltpu.make_async_copy(whole, whole, recv_sem.at[n]).wait()

    needs = {3: ("delta",), 4: (0, 1, 2, 3), 5: ("status",), 6: ("slack",), 7: ("net",), 8: ("ang",)}
    for n in (0, 1, 2, 4, 3, 5, 6, 7, 8):
        loaded(*needs.get(n, ()))
        send(n, *groups[n][:2])

    take(1, idx.at[core])
    idx_out = pltpu.make_async_remote_copy(
        src_ref=idx.at[core],
        dst_ref=idx.at[core],
        send_sem=pass_send.at[0],
        recv_sem=pass_recv.at[0],
        device_id=(partner, rank),
        device_id_type=MESH,
    )
    idx_out.start()
    take(0, base_z)
    group = planes // ranks
    home = base_all.at[lax.rem(me, group), :, :, me // group, :]
    pltpu.make_async_copy(base_z, home, base_recv).start()

    def spread(d, carry):
        pltpu.make_async_remote_copy(
            src_ref=base_z,
            dst_ref=home,
            send_sem=base_send,
            recv_sem=base_recv,
            device_id=(lax.rem(me + d, planes), rank),
            device_id_type=MESH,
        ).start()
        return carry

    lax.fori_loop(1, planes, spread, 0)

    loaded("zdual")
    comp_sq = jnp.zeros((ranks, LANES), F32)
    for t in range(line_tiles):
        cols = slice(t * LANES, (t + 1) * LANES)
        comp = status_v[:, cols].astype(F32) * (zdual_v[:, cols] * slack_v[:, cols] - 0.01)
        comp_sq += comp * comp
    comp_sum = jnp.sum(comp_sq, axis=1, keepdims=True)
    comp_row = jnp.sum(jnp.where(lane8 == row8 + 8, comp_sum, 0.0), axis=0, keepdims=True)

    take(2, mult_all)
    pltpu.make_async_copy(idx.at[1 - core], idx.at[1 - core], pass_recv.at[0]).wait()

    row16 = lax.broadcasted_iota(I32, (16, LANES), 0)
    ramp16 = row16.astype(F32).astype(BF16)
    none16, one16 = jnp.zeros((16, LANES), BF16), jnp.ones((16, LANES), BF16)
    high_row = [row8 * bus_tiles + t for t in range(bus_tiles)]
    n_rows = ranks * bus_tiles

    def one_hot(low, tiles):
        low = jnp.broadcast_to(low.astype(F32), (16, LANES)).astype(BF16)
        return jnp.concatenate(
            [jnp.where(low == ramp16 + BF16(16 * t), one16, none16) for t in range(tiles)], 0
        )

    def stack(q, tile):
        for t in range(0, bus_tiles, 2):
            both = jnp.concatenate([tile(t), tile(t + 1)], 0)
            coarse = both.astype(BF16)
            rows = slice(q * n_rows + ranks * t, q * n_rows + ranks * (t + 2))
            stacked[rows, 0:LANES] = coarse
            stacked[rows, LANES:] = (both - coarse.astype(F32)).astype(BF16)

    def by_matmul(k, count, store):
        for e in range(2):
            out = [jnp.zeros((ranks, LANES), F32) for _ in range(count)]
            for s in range(0, ranks, 2):
                hot, high = [], []
                for n in range(2):
                    bus = idx[e, k, s + n : s + n + 1, :]
                    high.append(jnp.broadcast_to(bus >> 7, (ranks, LANES)))
                    hot.append(one_hot(bus & 127, LANES // 16))
                hot = jnp.concatenate(hot, 1)
                rows = jnp.dot(
                    stacked[0 : count * n_rows, :],
                    jnp.concatenate([hot, hot], 0),
                    preferred_element_type=F32,
                )
                for n in range(2):
                    for q in range(count):
                        acc = jnp.zeros((ranks, LANES), F32)
                        for t in range(bus_tiles):
                            first = q * n_rows + ranks * t
                            part = rows[first : first + ranks, n * LANES : (n + 1) * LANES]
                            acc = jnp.where(high[n] == high_row[t], part, acc)
                        for step in (4, 2, 1):
                            acc = acc + pltpu.roll(acc, step, 0)
                        out[q] = jnp.where(row8 == s + n, acc, out[q])
            for q in range(count):
                store(e, q, out[q])

    def by_permute(k, store):
        for e in range(2):
            bus = idx[e, k]
            high, low = bus >> 7, bus & 127
            found = jnp.zeros((ranks, LANES), F32)
            for h in range(n_rows):
                r, t = h // bus_tiles, h % bus_tiles
                row = jnp.broadcast_to(angles[r : r + 1, t * LANES : (t + 1) * LANES], (ranks, LANES))
                got = jnp.take_along_axis(row, low, axis=1, mode="promise_in_bounds")
                found = jnp.where(high == h, got, found)
            store(e, found)

    for q in range(2):
        stack(q, lambda t: mult_all[q, :, t * LANES : (t + 1) * LANES])

    def gather_mult(k, carry):
        def store(e, q, value):
            ends[4 * e + 2 + q, k] = value

        by_matmul(k, 2, store)
        return carry

    middle = line_tiles // 3
    lax.fori_loop(0, middle, gather_mult, 0, unroll=True)
    take(4, coef.at[quad])
    for d in range(1, 4):
        pltpu.make_async_remote_copy(
            src_ref=coef.at[quad],
            dst_ref=coef.at[quad],
            send_sem=pass_send.at[1],
            recv_sem=pass_recv.at[1],
            device_id=(me - quad + lax.rem(quad + d, 4), rank),
            device_id_type=MESH,
        ).start()
    lax.fori_loop(middle, line_tiles, gather_mult, 0, unroll=True)

    take(3, delta_all)
    pltpu.make_async_copy(base_all, base_all, base_recv).wait()
    for q in range(2):
        tiles = [jnp.zeros((ranks, LANES), F32) for _ in range(bus_tiles)]
        for p in range(nbus // piece):
            rows = base_all[p // ranks, p % ranks, q]
            t, off = p * piece // LANES, p * piece % LANES
            moved = pltpu.roll(rows, off, 1) if off else rows
            tiles[t] = jnp.where((lane8 >= off) & (lane8 < off + piece), moved, tiles[t])
            if off + piece > LANES:
                tiles[t + 1] = jnp.where(lane8 < off + piece - LANES, moved, tiles[t + 1])
        for t in range(bus_tiles):
            cols = slice(t * LANES, (t + 1) * LANES)
            tiles[t] = tiles[t] + delta_all[q, :, cols]
            if q == 1:
                angles[:, cols] = tiles[t]
        if q == 0:
            stack(0, lambda t: tiles[t] - 1.0)

    def gather_angle(k):
        def store(e, value):
            ends[4 * e + 1, k] = value

        by_permute(k, store)

    def gather_size(k):
        def store(e, q, value):
            ends[4 * e, k] = value + 1.0

        by_matmul(k, 1, store)

    late = 4
    early = line_tiles - late

    def gather_both(k, carry):
        gather_angle(k)
        gather_size(k)
        return carry

    def gather_rest(k, carry):
        gather_size(k)
        return carry

    lax.fori_loop(0, early, gather_both, 0, unroll=True)
    lax.fori_loop(early, line_tiles, gather_rest, 0, unroll=True)

    pltpu.make_async_copy(coef.at[0:3], coef.at[0:3], pass_recv.at[1]).wait()
    take(5, status_all)

    def flows(k):
        cols = pl.ds(pl.multiple_of(k * LANES, LANES), LANES)
        vf, af, mpf, mqf = (ends[q, k] for q in range(4))
        vt, at, mpt, mqt = (ends[4 + q, k] for q in range(4))
        g, b, h = (coef[q, k] for q in range(3))
        live = status_all[:, cols].astype(F32)
        diff = af - at
        cs, sn = jnp.cos(diff), jnp.sin(diff)
        u = vf * vt
        gcs, gsn, bcs, bsn = g * cs, g * sn, b * cs, b * sn
        pf = (g * vf * vf - u * (gcs + bsn)) * live
        qf = (-(b + h) * vf * vf - u * (gsn - bcs)) * live
        pt = (g * vt * vt - u * (gcs - bsn)) * live
        qt = (-(b + h) * vt * vt + u * (gsn + bcs)) * live
        fd = u * (mpf * (gsn - bcs) - mqf * (gcs + bsn) + mpt * (gsn + bcs) + mqt * (gcs - bsn)) * live
        for n, v in enumerate((pf, qf, fd, pt, qt, -fd)):
            terms[n, k] = v

    per = nbus // 256
    high_of = [((row16 & 7) * per + j).astype(F32).astype(BF16) for j in range(per)]
    sums[...] = jnp.zeros_like(sums)

    def scatter(k):
        for s in range(ranks):
            left, right = [], []
            for e in range(2):
                at_bus = idx[e, k, s : s + 1, :]
                high = jnp.broadcast_to((at_bus >> 8).astype(F32), (16, LANES)).astype(BF16)
                vals = []
                for r in range(3):
                    v = terms[3 * e + r, k, s : s + 1, :]
                    coarse = v.astype(BF16).astype(F32)
                    fine = v - coarse
                    vals.append(
                        jnp.concatenate(
                            [jnp.broadcast_to(coarse, (8, LANES)), jnp.broadcast_to(fine, (8, LANES))], 0
                        ).astype(BF16)
                    )
                rows = []
                for j in range(per):
                    here = high == high_of[j]
                    rows += [jnp.where(here, v, none16) for v in vals]
                left.append(jnp.concatenate(rows, 0))
                right.append(one_hot(at_bus & 255, 16))
            sums[...] += lax.dot_general(
                jnp.concatenate(left, 1),
                jnp.concatenate(right, 1),
                (((1,), (1,)), ((), ())),
                preferred_element_type=F32,
            )

    def first_steps(k, carry):
        gather_angle(k + early)
        flows(k)
        scatter(k)
        return carry

    def other_steps(k, carry):
        flows(k)
        scatter(k)
        return carry

    lax.fori_loop(0, late, first_steps, 0, unroll=True)
    lax.fori_loop(late, line_tiles, other_steps, 0, unroll=True)

    take(6, slack_all)
    limit_sq = jnp.zeros((ranks, LANES), F32)
    for k in range(line_tiles):
        cols = slice(k * LANES, (k + 1) * LANES)
        pf, qf = terms[0, k], terms[1, k]
        live = status_all[:, cols].astype(F32)
        lim = live * (pf * pf + qf * qf + slack_all[:, cols] - coef[3, k] * coef[3, k])
        limit_out[:, cols] = lim
        limit_sq += lim * lim

    take(7, net_all)
    take(8, ang_all)
    mis_sq, dual_sq = jnp.zeros((ranks, 256), F32), jnp.zeros((ranks, 256), F32)
    for j in range(per):
        cols = slice(256 * j, 256 * (j + 1))
        for r in range(3):
            first = (3 * j + r) * 16
            got = sums[first : first + 8, :] + sums[first + 8 : first + 16, :]
            if r < 2:
                out = got - net_all[r, :, cols]
                mis_out[r, :, cols] = out
                mis_sq += out * out
            else:
                out = got + ang_all[:, cols]
                dual_out[:, cols] = out
                dual_sq += out * out

    mine = comp_row
    for n, part in enumerate((mis_sq, dual_sq, limit_sq)):
        mine = jnp.where(lane8[0:1] == n, jnp.sum(part, keepdims=True), mine)
    sq_mine[...] = mine
    n_limit, n_mis, n_dual, n_sq = (len(groups) + n for n in range(4))
    send(n_sq, lambda s: sq_mine, lambda r: sq_all.at[r])
    send(n_mis, lambda s: mis_out.at[:, s, :], lambda r: mismatch.at[r])
    send(n_dual, lambda s: dual_out.at[s], lambda r: dual.at[r])
    send(n_limit, lambda s: limit_out.at[s], lambda r: limit.at[r])

    take(n_sq, sq_all)
    every = sq_all[:, 0, :]
    group_sum = jnp.sum(every, axis=0, keepdims=True)
    tot_mine[...] = group_sum
    pltpu.make_async_copy(tot_mine, tot_all.at[me], tot_recv).start()

    def share(d, carry):
        pltpu.make_async_remote_copy(
            src_ref=tot_mine,
            dst_ref=tot_all.at[me],
            send_sem=tot_send,
            recv_sem=tot_recv,
            device_id=(lax.rem(me + d, planes), rank),
            device_id_type=MESH,
        ).start()
        return carry

    lax.fori_loop(1, planes, share, 0)
    comp_of = jnp.sum(jnp.where(lane8 == row8 + 8, group_sum, 0.0), axis=1, keepdims=True)
    norms[...] = jnp.sqrt(jnp.where(lane8 == 3, comp_of, jnp.where(lane8 < 3, every, 0.0)))
    take(n_limit, limit)
    take(n_mis, mismatch)
    take(n_dual, dual)
    idx_out.wait_send()
    pltpu.make_async_copy(coef.at[0:3], coef.at[0:3], pass_send.at[1]).wait()
    for n, (_, _, dest) in enumerate(groups):
        sent(send_sem.at[n], dest, ranks)
    for n, dest in ((n_limit, limit), (n_mis, mismatch), (n_dual, dual), (n_sq, sq_all)):
        sent(send_sem.at[n], dest, ranks)
    part = base_all.at[:, :, :, 0 : ranks - 1, :]
    pltpu.make_async_copy(part, part, base_send).wait()
    part = base_all.at[0 : group - 1, :, :, ranks - 1, :]
    pltpu.make_async_copy(part, part, base_send).wait()
    pltpu.make_async_copy(tot_all, tot_all, tot_recv).wait()
    whole = jnp.sum(tot_all[:, 0, :], axis=0, keepdims=True)
    lane1 = lane8[0:1]
    comp_whole = jnp.sum(jnp.where((lane1 >= 8) & (lane1 < 8 + ranks), whole, 0.0), axis=1, keepdims=True)
    whole = jnp.where(lane1 == 3, comp_whole, jnp.where(lane1 < 3, whole, 0.0))
    total[...] = jnp.sqrt(whole / (planes * ranks))
    part = tot_all.at[0 : planes - 1]
    pltpu.make_async_copy(part, part, tot_send).wait()


def sent(sem, dest, ranks):
    dim = len(dest.shape) - 1 - dest.shape[::-1].index(ranks)
    part = dest.at[(slice(None),) * dim + (slice(0, ranks - 1),)]
    pltpu.make_async_copy(part, part, sem).wait()


def hand_out(norms, total, mis, dual, limit, norms_out, total_out, mis_out, dual_out, limit_out):
    mis_out[...] = mis[...]
    dual_out[...] = dual[...]
    limit_out[...] = limit[...]
    norms_out[...] = norms[...].T[0:4, :]
    total_out[...] = total[:, 0:4]


def per_device(
    base_vm,
    base_va,
    delta_state,
    multipliers,
    net_inj,
    ang_grad,
    from_bus,
    to_bus,
    status,
    conduct,
    suscept,
    charging,
    rating,
    slack,
    zdual,
):
    planes, ranks = lax.axis_size("ctg"), lax.axis_size("br")
    nscen, _, nbus = delta_state.shape
    nline = status.shape[1]
    tiles = nline // LANES
    hbm = pl.BlockSpec(memory_space=pl.ANY)
    vmem = pl.BlockSpec(memory_space=pltpu.VMEM)
    V = pltpu.VMEM
    bus, line, deep = (ranks, nbus), (ranks, nline), (tiles, ranks, LANES)
    sem = pltpu.SemaphoreType.DMA
    grid = lambda a: a.reshape(tiles, LANES)
    results = pl.pallas_call(
        functools.partial(kernel, planes, ranks),
        out_shape=(
            V((nscen, 2, nbus), F32),
            V((nscen, nbus), F32),
            V((nscen, nline), F32),
            V((nscen, LANES), F32),
            V((1, LANES), F32),
        ),
        in_specs=[hbm] * 15,
        out_specs=(vmem,) * 5,
        scratch_shapes=[
            V((2, tiles, LANES), I32),
            V((4, tiles, LANES), F32),
            V((nscen, 2, nbus), F32),
            V((nscen, 2, nbus), F32),
            V((nscen, 2, nbus), F32),
            V((nscen, nbus), F32),
            V((nscen, nline), I32),
            V((nscen, nline), F32),
            V((nscen, nline), F32),
            pltpu.SMEM((2, base_vm.shape[0]), F32),
            V((2, LANES), F32),
            V((ranks, 2, LANES), F32),
            V((planes // ranks, ranks, 2, ranks, LANES), F32),
            V((2,) + deep, I32),
            V((4,) + deep, F32),
            V((2,) + bus, F32),
            V((2,) + bus, F32),
            V((2,) + bus, F32),
            V(bus, F32),
            V(line, I32),
            V(line, F32),
            V(bus, F32),
            V((2 * nbus // LANES * ranks, 2 * LANES), BF16),
            V((8,) + deep, F32),
            V((6,) + deep, F32),
            V((240, 256), F32),
            V((2,) + bus, F32),
            V(bus, F32),
            V(line, F32),
            V((1, LANES), F32),
            V((ranks, 1, LANES), F32),
            V((1, LANES), F32),
            V((planes, 1, LANES), F32),
            sem((15,)),
            sem((13,)),
            sem((13,)),
            sem((2,)),
            sem((2,)),
            sem,
            sem,
            sem,
            sem,
        ],
        compiler_params=pltpu.CompilerParams(collective_id=0, has_side_effects=True),
        name="residuals",
    )(
        base_vm,
        base_va,
        grid(from_bus),
        grid(to_bus),
        grid(conduct),
        grid(suscept),
        grid(charging),
        grid(rating),
        delta_state,
        multipliers,
        net_inj,
        ang_grad,
        status,
        slack,
        zdual,
    )
    mis, dual, limit, norms, total = (pltpu.with_memory_space_constraint(r, V) for r in results)
    norms, total, mis, dual, limit = pl.pallas_call(
        hand_out,
        out_shape=(
            jax.ShapeDtypeStruct((4, nscen), F32),
            jax.ShapeDtypeStruct((1, 4), F32),
            jax.ShapeDtypeStruct((nscen, 2, nbus), F32),
            jax.ShapeDtypeStruct((nscen, nbus), F32),
            jax.ShapeDtypeStruct((nscen, nline), F32),
        ),
        in_specs=[vmem] * 5,
        out_specs=(vmem,) * 5,
        name="hand_out",
    )(norms, total, mis, dual, limit)
    return mis, dual, limit, norms.T, total.reshape(4)


def solution(mesh):
    placed = (
        P(("ctg", "br")),
        P(("ctg", "br")),
        P("ctg", None, "br"),
        P("ctg", None, "br"),
        P("ctg", None, "br"),
        P("ctg", "br"),
        P("br"),
        P("br"),
        P("ctg", "br"),
        P("br"),
        P("br"),
        P("br"),
        P("br"),
        P("ctg", "br"),
        P("ctg", "br"),
    )
    return jax.shard_map(
        per_device,
        mesh=mesh,
        in_specs=placed,
        out_specs=(P("ctg", None, "br"), P("ctg", "br"), P("ctg", "br"), P("ctg", None), P()),
        check_vma=False,
    )
```

```python
import functools

import jax
import jax.numpy as jnp
from jax import lax
from jax.experimental import pallas as pl
from jax.experimental.pallas import tpu as pltpu
from jax.sharding import PartitionSpec as P

F32, I32, BF16 = jnp.float32, jnp.int32, jnp.bfloat16
LANES = 128
MESH = pl.DeviceIdType.MESH


def kernel(
    planes,
    ranks,
    base_vm,
    base_va,
    from_bus,
    to_bus,
    conduct,
    suscept,
    charging,
    rating,
    delta,
    mult,
    net,
    ang,
    status,
    slack,
    zdual,
    mismatch,
    dual,
    limit,
    norms,
    total,
    lines_i,
    lines_f,
    delta_v,
    mult_v,
    net_v,
    ang_v,
    status_v,
    slack_v,
    zdual_v,
    base_s,
    base_v,
    base_z,
    base_all,
    idx,
    coef,
    mult_all,
    delta_all,
    net_all,
    ang_all,
    status_all,
    slack_all,
    angles,
    stacked,
    ends,
    terms,
    sums,
    mis_out,
    dual_out,
    limit_out,
    sq_mine,
    sq_all,
    tot_mine,
    tot_all,
    load_sem,
    send_sem,
    recv_sem,
    pass_send,
    pass_recv,
    base_send,
    base_recv,
    tot_send,
    tot_recv,
):
    me = lax.axis_index("ctg")
    rank = lax.axis_index("br")
    core = lax.rem(me, 2)
    partner = me + 1 - 2 * core
    nbus = delta.shape[2]
    nline = status.shape[1]
    bus_tiles, line_tiles = nbus // LANES, nline // LANES

    loads = {}

    def load(name, source, place):
        loads[name] = pltpu.make_async_copy(source, place, load_sem.at[len(loads)])
        loads[name].start()

    def loaded(*names):
        for name in names:
            loads[name].wait()

    load("from", from_bus, lines_i.at[0])
    load("to", to_bus, lines_i.at[1])
    load("mult", mult, mult_v)
    load("vm", base_vm, base_s.at[0])
    load("va", base_va, base_s.at[1])
    load("delta", delta, delta_v)

    barrier = pltpu.get_barrier_semaphore()
    for d in range(1, ranks):
        pl.semaphore_signal(barrier, 1, device_id=(me, lax.rem(rank + d, ranks)), device_id_type=MESH)

    def greet(d, carry):
        pl.semaphore_signal(barrier, 1, device_id=(lax.rem(me + d, planes), rank), device_id_type=MESH)
        return carry

    lax.fori_loop(1, planes, greet, 0)

    for n, ref in enumerate((conduct, suscept, charging, rating)):
        load(n, ref, lines_f.at[n])
    load("status", status, status_v)
    load("slack", slack, slack_v)
    load("net", net, net_v)
    load("ang", ang, ang_v)
    load("zdual", zdual, zdual_v)

    lane8 = lax.broadcasted_iota(I32, (ranks, LANES), 1)
    row8 = lax.broadcasted_iota(I32, (ranks, LANES), 0)
    piece = base_vm.shape[0]
    loaded("vm", "va")
    for q in range(2):
        spread_out = jnp.zeros((1, LANES), F32)
        for n in range(piece):
            spread_out = jnp.where(lane8[0:1] == n, base_s[q, n], spread_out)
        base_v[q : q + 1, :] = spread_out
    loaded("from", "to", "mult")

    pl.semaphore_wait(barrier, ranks - 1 + planes - 1)

    quad = lax.rem(me, 4)
    groups = (
        (lambda s: base_v, lambda r: base_z.at[r], base_z),
        (lambda s: lines_i.at[core], lambda r: idx.at[core, :, r, :], idx.at[core]),
        (lambda s: mult_v.at[s], lambda r: mult_all.at[:, r, :], mult_all),
        (lambda s: delta_v.at[s], lambda r: delta_all.at[:, r, :], delta_all),
        (lambda s: lines_f.at[quad], lambda r: coef.at[quad, :, r, :], coef.at[quad]),
        (lambda s: status_v.at[s], lambda r: status_all.at[r], status_all),
        (lambda s: slack_v.at[s], lambda r: slack_all.at[r], slack_all),
        (lambda s: net_v.at[s], lambda r: net_all.at[:, r, :], net_all),
        (lambda s: ang_v.at[s], lambda r: ang_all.at[r], ang_all),
    )

    def send(n, source, place):
        pltpu.make_async_copy(source(rank), place(rank), recv_sem.at[n]).start()
        for d in (4, 3, 5, 2, 6, 1, 7):
            peer = lax.rem(rank + d, ranks)
            pltpu.make_async_remote_copy(
                src_ref=source(peer),
                dst_ref=place(rank),
                send_sem=send_sem.at[n],
                recv_sem=recv_sem.at[n],
                device_id=(me, peer),
                device_id_type=MESH,
            ).start()

    def take(n, whole):
        pltpu.make_async_copy(whole, whole, recv_sem.at[n]).wait()

    needs = {3: ("delta",), 4: (0, 1, 2, 3), 5: ("status",), 6: ("slack",), 7: ("net",), 8: ("ang",)}
    for n in (0, 1, 2, 4, 3, 5, 6, 7, 8):
        loaded(*needs.get(n, ()))
        send(n, *groups[n][:2])

    take(1, idx.at[core])
    idx_out = pltpu.make_async_remote_copy(
        src_ref=idx.at[core],
        dst_ref=idx.at[core],
        send_sem=pass_send.at[0],
        recv_sem=pass_recv.at[0],
        device_id=(partner, rank),
        device_id_type=MESH,
    )
    idx_out.start()
    take(0, base_z)
    group = planes // ranks
    home = base_all.at[lax.rem(me, group), :, :, me // group, :]
    pltpu.make_async_copy(base_z, home, base_recv).start()

    def spread(d, carry):
        pltpu.make_async_remote_copy(
            src_ref=base_z,
            dst_ref=home,
            send_sem=base_send,
            recv_sem=base_recv,
            device_id=(lax.rem(me + d, planes), rank),
            device_id_type=MESH,
        ).start()
        return carry

    lax.fori_loop(1, planes, spread, 0)

    loaded("zdual")
    comp_sq = jnp.zeros((ranks, LANES), F32)
    for t in range(line_tiles):
        cols = slice(t * LANES, (t + 1) * LANES)
        comp = status_v[:, cols].astype(F32) * (zdual_v[:, cols] * slack_v[:, cols] - 0.01)
        comp_sq += comp * comp
    comp_sum = jnp.sum(comp_sq, axis=1, keepdims=True)
    comp_row = jnp.sum(jnp.where(lane8 == row8 + 8, comp_sum, 0.0), axis=0, keepdims=True)

    take(2, mult_all)
    pltpu.make_async_copy(idx.at[1 - core], idx.at[1 - core], pass_recv.at[0]).wait()

    row16 = lax.broadcasted_iota(I32, (16, LANES), 0)
    ramp16 = row16.astype(F32).astype(BF16)
    none16, one16 = jnp.zeros((16, LANES), BF16), jnp.ones((16, LANES), BF16)
    high_row = [row8 * bus_tiles + t for t in range(bus_tiles)]
    n_rows = ranks * bus_tiles

    def one_hot(low, tiles):
        low = jnp.broadcast_to(low.astype(F32), (16, LANES)).astype(BF16)
        return jnp.concatenate(
            [jnp.where(low == ramp16 + BF16(16 * t), one16, none16) for t in range(tiles)], 0
        )

    def stack(q, tile):
        for t in range(0, bus_tiles, 2):
            both = jnp.concatenate([tile(t), tile(t + 1)], 0)
            coarse = both.astype(BF16)
            rows = slice(q * n_rows + ranks * t, q * n_rows + ranks * (t + 2))
            stacked[rows, 0:LANES] = coarse
            stacked[rows, LANES:] = (both - coarse.astype(F32)).astype(BF16)

    def by_matmul(k, count, store):
        for e in range(2):
            out = [jnp.zeros((ranks, LANES), F32) for _ in range(count)]
            for s in range(0, ranks, 2):
                hot, high = [], []
                for n in range(2):
                    bus = idx[e, k, s + n : s + n + 1, :]
                    high.append(jnp.broadcast_to(bus >> 7, (ranks, LANES)))
                    hot.append(one_hot(bus & 127, LANES // 16))
                hot = jnp.concatenate(hot, 1)
                rows = jnp.dot(
                    stacked[0 : count * n_rows, :],
                    jnp.concatenate([hot, hot], 0),
                    preferred_element_type=F32,
                )
                for n in range(2):
                    for q in range(count):
                        acc = jnp.zeros((ranks, LANES), F32)
                        for t in range(bus_tiles):
                            first = q * n_rows + ranks * t
                            part = rows[first : first + ranks, n * LANES : (n + 1) * LANES]
                            acc = jnp.where(high[n] == high_row[t], part, acc)
                        for step in (4, 2, 1):
                            acc = acc + pltpu.roll(acc, step, 0)
                        out[q] = jnp.where(row8 == s + n, acc, out[q])
            for q in range(count):
                store(e, q, out[q])

    def by_permute(k, store):
        for e in range(2):
            bus = idx[e, k]
            high, low = bus >> 7, bus & 127
            found = jnp.zeros((ranks, LANES), F32)
            for h in range(n_rows):
                r, t = h // bus_tiles, h % bus_tiles
                row = jnp.broadcast_to(angles[r : r + 1, t * LANES : (t + 1) * LANES], (ranks, LANES))
                got = jnp.take_along_axis(row, low, axis=1, mode="promise_in_bounds")
                found = jnp.where(high == h, got, found)
            store(e, found)

    for q in range(2):
        stack(q, lambda t: mult_all[q, :, t * LANES : (t + 1) * LANES])

    def gather_mult(k, carry):
        def store(e, q, value):
            ends[4 * e + 2 + q, k] = value

        by_matmul(k, 2, store)
        return carry

    middle = line_tiles // 3
    lax.fori_loop(0, middle, gather_mult, 0, unroll=True)
    take(4, coef.at[quad])
    for d in range(1, 4):
        pltpu.make_async_remote_copy(
            src_ref=coef.at[quad],
            dst_ref=coef.at[quad],
            send_sem=pass_send.at[1],
            recv_sem=pass_recv.at[1],
            device_id=(me - quad + lax.rem(quad + d, 4), rank),
            device_id_type=MESH,
        ).start()
    lax.fori_loop(middle, line_tiles, gather_mult, 0, unroll=True)

    take(3, delta_all)
    pltpu.make_async_copy(base_all, base_all, base_recv).wait()
    for q in range(2):
        tiles = [jnp.zeros((ranks, LANES), F32) for _ in range(bus_tiles)]
        for p in range(nbus // piece):
            rows = base_all[p // ranks, p % ranks, q]
            t, off = p * piece // LANES, p * piece % LANES
            moved = pltpu.roll(rows, off, 1) if off else rows
            tiles[t] = jnp.where((lane8 >= off) & (lane8 < off + piece), moved, tiles[t])
            if off + piece > LANES:
                tiles[t + 1] = jnp.where(lane8 < off + piece - LANES, moved, tiles[t + 1])
        for t in range(bus_tiles):
            cols = slice(t * LANES, (t + 1) * LANES)
            tiles[t] = tiles[t] + delta_all[q, :, cols]
            if q == 1:
                angles[:, cols] = tiles[t]
        if q == 0:
            stack(0, lambda t: tiles[t] - 1.0)

    def gather_angle(k):
        def store(e, value):
            ends[4 * e + 1, k] = value

        by_permute(k, store)

    def gather_size(k):
        def store(e, q, value):
            ends[4 * e, k] = value + 1.0

        by_matmul(k, 1, store)

    late = 6
    early = line_tiles - late

    def gather_both(k, carry):
        gather_angle(k)
        gather_size(k)
        return carry

    def gather_rest(k, carry):
        gather_size(k)
        return carry

    lax.fori_loop(0, early, gather_both, 0, unroll=True)
    lax.fori_loop(early, line_tiles, gather_rest, 0, unroll=True)

    pltpu.make_async_copy(coef.at[0:3], coef.at[0:3], pass_recv.at[1]).wait()
    take(5, status_all)

    def flows(k):
        cols = pl.ds(pl.multiple_of(k * LANES, LANES), LANES)
        vf, af, mpf, mqf = (ends[q, k] for q in range(4))
        vt, at, mpt, mqt = (ends[4 + q, k] for q in range(4))
        g, b, h = (coef[q, k] for q in range(3))
        live = status_all[:, cols].astype(F32)
        diff = af - at
        cs, sn = jnp.cos(diff), jnp.sin(diff)
        u = vf * vt
        gcs, gsn, bcs, bsn = g * cs, g * sn, b * cs, b * sn
        pf = (g * vf * vf - u * (gcs + bsn)) * live
        qf = (-(b + h) * vf * vf - u * (gsn - bcs)) * live
        pt = (g * vt * vt - u * (gcs - bsn)) * live
        qt = (-(b + h) * vt * vt + u * (gsn + bcs)) * live
        fd = u * (mpf * (gsn - bcs) - mqf * (gcs + bsn) + mpt * (gsn + bcs) + mqt * (gcs - bsn)) * live
        for n, v in enumerate((pf, qf, fd, pt, qt, -fd)):
            terms[n, k] = v

    per = nbus // 256
    high_of = [((row16 & 7) * per + j).astype(F32).astype(BF16) for j in range(per)]
    sums[...] = jnp.zeros_like(sums)

    def scatter(k):
        for s in range(ranks):
            left, right = [], []
            for e in range(2):
                at_bus = idx[e, k, s : s + 1, :]
                high = jnp.broadcast_to((at_bus >> 8).astype(F32), (16, LANES)).astype(BF16)
                vals = []
                for r in range(3):
                    v = terms[3 * e + r, k, s : s + 1, :]
                    coarse = v.astype(BF16).astype(F32)
                    fine = v - coarse
                    vals.append(
                        jnp.concatenate(
                            [jnp.broadcast_to(coarse, (8, LANES)), jnp.broadcast_to(fine, (8, LANES))], 0
                        ).astype(BF16)
                    )
                rows = []
                for j in range(per):
                    here = high == high_of[j]
                    rows += [jnp.where(here, v, none16) for v in vals]
                left.append(jnp.concatenate(rows, 0))
                right.append(one_hot(at_bus & 255, 16))
            sums[...] += lax.dot_general(
                jnp.concatenate(left, 1),
                jnp.concatenate(right, 1),
                (((1,), (1,)), ((), ())),
                preferred_element_type=F32,
            )

    def first_steps(k, carry):
        gather_angle(k + early)
        flows(k)
        scatter(k)
        return carry

    def other_steps(k, carry):
        flows(k)
        scatter(k)
        return carry

    lax.fori_loop(0, late, first_steps, 0, unroll=True)
    lax.fori_loop(late, line_tiles, other_steps, 0, unroll=True)

    take(6, slack_all)
    limit_sq = jnp.zeros((ranks, LANES), F32)
    for k in range(line_tiles):
        cols = slice(k * LANES, (k + 1) * LANES)
        pf, qf = terms[0, k], terms[1, k]
        live = status_all[:, cols].astype(F32)
        lim = live * (pf * pf + qf * qf + slack_all[:, cols] - coef[3, k] * coef[3, k])
        limit_out[:, cols] = lim
        limit_sq += lim * lim

    take(7, net_all)
    take(8, ang_all)
    mis_sq, dual_sq = jnp.zeros((ranks, 256), F32), jnp.zeros((ranks, 256), F32)
    for j in range(per):
        cols = slice(256 * j, 256 * (j + 1))
        for r in range(3):
            first = (3 * j + r) * 16
            got = sums[first : first + 8, :] + sums[first + 8 : first + 16, :]
            if r < 2:
                out = got - net_all[r, :, cols]
                mis_out[r, :, cols] = out
                mis_sq += out * out
            else:
                out = got + ang_all[:, cols]
                dual_out[:, cols] = out
                dual_sq += out * out

    mine = comp_row
    for n, part in enumerate((mis_sq, dual_sq, limit_sq)):
        mine = jnp.where(lane8[0:1] == n, jnp.sum(part, keepdims=True), mine)
    sq_mine[...] = mine
    n_limit, n_mis, n_dual, n_sq = (len(groups) + n for n in range(4))
    send(n_sq, lambda s: sq_mine, lambda r: sq_all.at[r])
    send(n_mis, lambda s: mis_out.at[:, s, :], lambda r: mismatch.at[r])
    send(n_dual, lambda s: dual_out.at[s], lambda r: dual.at[r])
    send(n_limit, lambda s: limit_out.at[s], lambda r: limit.at[r])

    take(n_sq, sq_all)
    every = sq_all[:, 0, :]
    group_sum = jnp.sum(every, axis=0, keepdims=True)
    tot_mine[...] = group_sum
    pltpu.make_async_copy(tot_mine, tot_all.at[me], tot_recv).start()

    def share(d, carry):
        pltpu.make_async_remote_copy(
            src_ref=tot_mine,
            dst_ref=tot_all.at[me],
            send_sem=tot_send,
            recv_sem=tot_recv,
            device_id=(lax.rem(me + d, planes), rank),
            device_id_type=MESH,
        ).start()
        return carry

    lax.fori_loop(1, planes, share, 0)
    comp_of = jnp.sum(jnp.where(lane8 == row8 + 8, group_sum, 0.0), axis=1, keepdims=True)
    norms[...] = jnp.sqrt(jnp.where(lane8 == 3, comp_of, jnp.where(lane8 < 3, every, 0.0)))
    take(n_limit, limit)
    take(n_mis, mismatch)
    take(n_dual, dual)
    idx_out.wait_send()
    pltpu.make_async_copy(coef.at[0:3], coef.at[0:3], pass_send.at[1]).wait()
    for n, (_, _, dest) in enumerate(groups):
        sent(send_sem.at[n], dest, ranks)
    for n, dest in ((n_limit, limit), (n_mis, mismatch), (n_dual, dual), (n_sq, sq_all)):
        sent(send_sem.at[n], dest, ranks)
    part = base_all.at[:, :, :, 0 : ranks - 1, :]
    pltpu.make_async_copy(part, part, base_send).wait()
    part = base_all.at[0 : group - 1, :, :, ranks - 1, :]
    pltpu.make_async_copy(part, part, base_send).wait()
    pltpu.make_async_copy(tot_all, tot_all, tot_recv).wait()
    whole = jnp.sum(tot_all[:, 0, :], axis=0, keepdims=True)
    lane1 = lane8[0:1]
    comp_whole = jnp.sum(jnp.where((lane1 >= 8) & (lane1 < 8 + ranks), whole, 0.0), axis=1, keepdims=True)
    whole = jnp.where(lane1 == 3, comp_whole, jnp.where(lane1 < 3, whole, 0.0))
    total[...] = jnp.sqrt(whole / (planes * ranks))
    part = tot_all.at[0 : planes - 1]
    pltpu.make_async_copy(part, part, tot_send).wait()


def sent(sem, dest, ranks):
    dim = len(dest.shape) - 1 - dest.shape[::-1].index(ranks)
    part = dest.at[(slice(None),) * dim + (slice(0, ranks - 1),)]
    pltpu.make_async_copy(part, part, sem).wait()


def hand_out(norms, total, mis, dual, limit, norms_out, total_out, mis_out, dual_out, limit_out):
    mis_out[...] = mis[...]
    dual_out[...] = dual[...]
    limit_out[...] = limit[...]
    norms_out[...] = norms[...].T[0:4, :]
    total_out[...] = total[:, 0:4]


def per_device(
    base_vm,
    base_va,
    delta_state,
    multipliers,
    net_inj,
    ang_grad,
    from_bus,
    to_bus,
    status,
    conduct,
    suscept,
    charging,
    rating,
    slack,
    zdual,
):
    planes, ranks = lax.axis_size("ctg"), lax.axis_size("br")
    nscen, _, nbus = delta_state.shape
    nline = status.shape[1]
    tiles = nline // LANES
    hbm = pl.BlockSpec(memory_space=pl.ANY)
    vmem = pl.BlockSpec(memory_space=pltpu.VMEM)
    V = pltpu.VMEM
    bus, line, deep = (ranks, nbus), (ranks, nline), (tiles, ranks, LANES)
    sem = pltpu.SemaphoreType.DMA
    grid = lambda a: a.reshape(tiles, LANES)
    results = pl.pallas_call(
        functools.partial(kernel, planes, ranks),
        out_shape=(
            V((nscen, 2, nbus), F32),
            V((nscen, nbus), F32),
            V((nscen, nline), F32),
            V((nscen, LANES), F32),
            V((1, LANES), F32),
        ),
        in_specs=[hbm] * 15,
        out_specs=(vmem,) * 5,
        scratch_shapes=[
            V((2, tiles, LANES), I32),
            V((4, tiles, LANES), F32),
            V((nscen, 2, nbus), F32),
            V((nscen, 2, nbus), F32),
            V((nscen, 2, nbus), F32),
            V((nscen, nbus), F32),
            V((nscen, nline), I32),
            V((nscen, nline), F32),
            V((nscen, nline), F32),
            pltpu.SMEM((2, base_vm.shape[0]), F32),
            V((2, LANES), F32),
            V((ranks, 2, LANES), F32),
            V((planes // ranks, ranks, 2, ranks, LANES), F32),
            V((2,) + deep, I32),
            V((4,) + deep, F32),
            V((2,) + bus, F32),
            V((2,) + bus, F32),
            V((2,) + bus, F32),
            V(bus, F32),
            V(line, I32),
            V(line, F32),
            V(bus, F32),
            V((2 * nbus // LANES * ranks, 2 * LANES), BF16),
            V((8,) + deep, F32),
            V((6,) + deep, F32),
            V((240, 256), F32),
            V((2,) + bus, F32),
            V(bus, F32),
            V(line, F32),
            V((1, LANES), F32),
            V((ranks, 1, LANES), F32),
            V((1, LANES), F32),
            V((planes, 1, LANES), F32),
            sem((15,)),
            sem((13,)),
            sem((13,)),
            sem((2,)),
            sem((2,)),
            sem,
            sem,
            sem,
            sem,
        ],
        compiler_params=pltpu.CompilerParams(collective_id=0, has_side_effects=True),
        name="residuals",
    )(
        base_vm,
        base_va,
        grid(from_bus),
        grid(to_bus),
        grid(conduct),
        grid(suscept),
        grid(charging),
        grid(rating),
        delta_state,
        multipliers,
        net_inj,
        ang_grad,
        status,
        slack,
        zdual,
    )
    mis, dual, limit, norms, total = (pltpu.with_memory_space_constraint(r, V) for r in results)
    norms, total, mis, dual, limit = pl.pallas_call(
        hand_out,
        out_shape=(
            jax.ShapeDtypeStruct((4, nscen), F32),
            jax.ShapeDtypeStruct((1, 4), F32),
            jax.ShapeDtypeStruct((nscen, 2, nbus), F32),
            jax.ShapeDtypeStruct((nscen, nbus), F32),
            jax.ShapeDtypeStruct((nscen, nline), F32),
        ),
        in_specs=[vmem] * 5,
        out_specs=(vmem,) * 5,
        name="hand_out",
    )(norms, total, mis, dual, limit)
    return mis, dual, limit, norms.T, total.reshape(4)


def solution(mesh):
    placed = (
        P(("ctg", "br")),
        P(("ctg", "br")),
        P("ctg", None, "br"),
        P("ctg", None, "br"),
        P("ctg", None, "br"),
        P("ctg", "br"),
        P("br"),
        P("br"),
        P("ctg", "br"),
        P("br"),
        P("br"),
        P("br"),
        P("br"),
        P("ctg", "br"),
        P("ctg", "br"),
    )
    return jax.shard_map(
        per_device,
        mesh=mesh,
        in_specs=placed,
        out_specs=(P("ctg", None, "br"), P("ctg", "br"), P("ctg", "br"), P("ctg", None), P()),
        check_vma=False,
    )
```
